256 devices in a mesh: replica: 64 (over z_hi, y, x, core), mp: 4 (over z_lo).
Axes of the slice: x: 4, y: 4, z: 8 (z_hi: 2, z_lo: 4; z = z_hi * 4 + z_lo), core: 2. Of those that a mesh axis runs over, the one named last changes fastest.
Arguments:
- pseudo_grad: bfloat16 [64, 2, 3072, 2048], P('replica', None, None, 'mp'), may hold values from -16 to 16
- outer_params: float32 [2, 3072, 2048], P(None, 'replica', 'mp'), may hold values from -6 to 6
- momentum: float32 [2, 3072, 2048], P(None, 'replica', 'mp'), may hold values from -3 to 3
- acts: bfloat16 [8192, 3072], P('replica', 'mp'), may hold values from -6 to 6
- queries: bfloat16 [8192, 2048], P('replica', 'mp'), may hold values from -6 to 6
- keys: bfloat16 [8192, 2048], P('replica', 'mp'), may hold values from -6 to 6
- doc_ids: int32 [8192], P('replica'), may hold values from 0 to 255, never falling along the last dimension, each value on 1 to 64 neighbouring positions
Outputs:
- new_outer: float32 [2, 3072, 2048], P(None, 'replica', 'mp')
- new_momentum: float32 [2, 3072, 2048], P(None, 'replica', 'mp')
- new_local: bfloat16 [64, 3072, 2048], P('replica', None, 'mp')
The draws below stay inside these ranges and needn't reach their ends.
Inputs may be any that keep to these rules, and one draw needn't show every extreme that they name: doc_ids never fall along the rows; each document covers 1 to 64 positions.
All inputs are finite; a program needn't handle non-finite values.
Results may differ from the reference program's by a relative error of at most 0.0037.
The reference program's roundings to bfloat16 on the way count: a program that leaves them out, or rounds other values in their place, can miss the bound.
Values may be sent and summed in bfloat16 or wider, within the bound.
No kernel may reach another device: no remote copies, remote signals or barrier semaphores. Data moves between devices by JAX's collectives and lax.ppermute only.
A program may use at most 64 MiB of HBM per device.

```python
import math
import jax
import jax.numpy as jnp
import numpy as np
from jax import lax

D = 3072
HD = 256
TOK = 128
HW = 2048
WORKERS = 64
TOKENS = 8192


def spiked(drawn, rng, source, target, parts, factor):
    def block_of(position):
        return (jnp.arange(drawn.shape[position]) // (drawn.shape[position] // parts)).reshape((-1,) + (1,) * (drawn.ndim - 1 - position))

    one_side = jax.random.permutation(rng, parts)[block_of(target)]
    far = (block_of(target) + parts // 2) % parts
    return jnp.where((block_of(source) == one_side) | (block_of(source) == far), factor * drawn, drawn)


def levels(stream_key, shape, split, least, largest):
    factor_of, own = 1.0, jax.random.fold_in(stream_key, 6)
    for dim, shards_of in split:
        draws = jnp.exp(jax.random.uniform(jax.random.fold_in(own, dim), (shards_of,), jnp.float32, least / len(split), largest / len(split)))
        factor_of = factor_of * jnp.repeat(draws, shape[dim] // shards_of).reshape([-1 if axis == dim else 1 for axis in range(len(shape))])
    return factor_of


def length_profile(amount, total, most, lean):
    loads = [(1 << 20) // math.isqrt(standing ** lean) + 1 for standing in range(2, amount + 1)]
    surplus, given = total - most - (amount - 1), [1] * (amount - 1)
    while surplus > 0:
        free = [i for i in range(amount - 1) if given[i] < most]
        whole, left = sum([loads[i] for i in free]), surplus
        for i in free:
            extra = min(most - given[i], max(1, left * loads[i] // whole), surplus)
            given[i] = given[i] + extra
            surplus = surplus - extra
    return np.array([most] + given)


def ragged(own_key, count, total, bound, slope):
    if count == 2:
        one = jax.random.randint(own_key, (), max(1, total - bound), min(bound, total - 1) + 1)
        return jnp.stack([one, total - one])
    tallies = jnp.asarray(length_profile(count, total, bound, slope), jnp.int32)
    pairs = (count - 1) // 2
    giver, sink = tallies[1:1 + 2 * pairs:2], tallies[2:2 + 2 * pairs:2]
    slack = jnp.minimum(giver - 1, bound - sink)
    moved = jax.random.randint(jax.random.fold_in(own_key, 1), (pairs,), 0, 1 << 20) % (slack + 1)
    tallies = tallies.at[1:1 + 2 * pairs:2].set(giver - moved).at[2:2 + 2 * pairs:2].set(sink + moved)
    return tallies[jax.random.permutation(jax.random.fold_in(own_key, 2), count)]


def gaussian(own_key, dims, scale, limit, shards=(), kind=jnp.bfloat16):
    entries = jax.random.normal(own_key, dims, jnp.float32) * scale
    if len(shards) > 0:
        entries = levels(own_key, dims, shards, -0.22, 0.18) * entries
    return jnp.clip(entries, min=-limit, max=limit).astype(kind)


def noise_with(own_key, dims, deviation, bound, split, heavy, dtype=jnp.bfloat16):
    entries = deviation * jax.random.normal(own_key, dims, jnp.float32)
    if split:
        entries = entries * levels(own_key, dims, split, -0.22, 0.18)
    return jnp.clip(spiked(entries, jax.random.fold_in(own_key, 3), *heavy), -bound, bound).astype(dtype)


def setup_inputs(seed: int = 0) -> dict:
    arg_keys = jax.random.split(jax.random.key(seed), 8)
    pseudo_grad = noise_with(arg_keys[0], (WORKERS, 2, D, HW), 1.0, 16.0, ((0, 64), (3, 4)), (0, 2, 64, 4.0))
    outer_params = gaussian(arg_keys[1], (2, D, HW), 1.0, 6.0, ((1, 64), (2, 4)), jnp.float32)
    momentum = gaussian(arg_keys[2], (2, D, HW), 0.3, 3.0, ((1, 64), (2, 4)), jnp.float32)
    acts = gaussian(arg_keys[3], (TOKENS, D), 1.0, 6.0, ((0, 64), (1, 4)))
    queries = gaussian(arg_keys[4], (TOKENS, HW), 1.0, 6.0, ((0, 64), (1, 4)))
    keys = gaussian(arg_keys[5], (TOKENS, HW), 1.0, 6.0, ((0, 64), (1, 4)))
    doc_ids = jnp.searchsorted(jnp.cumsum(ragged(arg_keys[6], TOKENS // 32, TOKENS, 64, 1)), jnp.arange(TOKENS), side="right").astype(jnp.int32)
    return {"pseudo_grad": pseudo_grad, "outer_params": outer_params, "momentum": momentum, "acts": acts, "queries": queries, "keys": keys, "doc_ids": doc_ids}


norm_eps = 1e-06
outer_rate = 0.7
outer_beta = 0.9
inner_rate = 0.1

def attend(query, key_rows, value_rows, doc_rows):
    count = query.shape[0]
    scores = jnp.einsum('qhd,khd->hqk', query, key_rows, preferred_element_type=jnp.float32) * query.shape[2] ** (-0.5)
    row_pos = lax.broadcasted_iota(jnp.int32, (count, count), 0)
    col_pos = lax.broadcasted_iota(jnp.int32, (count, count), 1)
    allowed = (row_pos >= col_pos) & (doc_rows[:, None] == doc_rows[None, :])
    scores = jnp.where(allowed[None], scores, -1e+30)
    probs = jax.nn.softmax(scores, axis=-1).astype(jnp.bfloat16)
    context = jnp.einsum('hqk,khd->qhd', probs, value_rows, preferred_element_type=jnp.float32)
    return context.astype(jnp.bfloat16)

def inner_step(weights, rows, query_rows, key_rows, doc_rows):
    count, width = rows.shape
    cols = weights.shape[2]
    heads_here = cols // HD
    rows_f = rows.astype(jnp.float32)
    normed = (rows_f * lax.rsqrt(lax.optimization_barrier(jnp.mean(rows_f * rows_f, axis=-1, keepdims=True)) + norm_eps)).astype(jnp.bfloat16)
    values = (jnp.dot(normed, weights[0], preferred_element_type=jnp.float32) * width ** (-0.5)).astype(jnp.bfloat16)
    query = query_rows.reshape(count, heads_here, HD)
    keyed = key_rows.reshape(count, heads_here, HD)

    def attn_fn(c):
        return attend(query, keyed, c, doc_rows)
    context, pullback = jax.vjp(attn_fn, values.reshape(count, heads_here, HD))
    ctx = context.reshape(count, cols)
    branch = jnp.dot(ctx, weights[1].T, preferred_element_type=jnp.float32) * cols ** (-0.5)
    dout = (rows_f + branch - jnp.roll(rows_f, -1, axis=0)).astype(jnp.bfloat16)
    dctx = (jnp.dot(dout, weights[1], preferred_element_type=jnp.float32) * cols ** (-0.5)).astype(jnp.bfloat16)
    pulled = pullback(dctx.reshape(count, heads_here, HD))[0].astype(jnp.bfloat16)
    grad = jnp.dot(normed.T, pulled.reshape(count, cols), preferred_element_type=jnp.float32) * width ** (-0.5)
    rms = jnp.sqrt(jnp.mean(grad * grad) + norm_eps)
    return (weights[0].astype(jnp.float32) - inner_rate * grad / rms).astype(jnp.bfloat16)

def reference(pseudo_grad, outer_params, momentum, acts, queries, keys, doc_ids):
    total = lax.fori_loop(0, WORKERS, lambda i, acc: acc + pseudo_grad[i].astype(jnp.float32), jnp.zeros(outer_params.shape, jnp.float32))
    delta = total / WORKERS
    new_momentum = outer_beta * momentum + delta
    new_outer = outer_params - outer_rate * (delta + outer_beta * new_momentum)
    weights = new_outer.astype(jnp.bfloat16)
    rows_all = acts.reshape(WORKERS, TOK, D)
    query_all = queries.reshape(WORKERS, TOK, HW)
    key_all = keys.reshape(WORKERS, TOK, HW)
    docs_all = doc_ids.reshape(WORKERS, TOK)
    new_local = lax.map(lambda group: inner_step(weights, group[0], group[1], group[2], group[3]), (rows_all, query_all, key_all, docs_all))
    return (new_outer, new_momentum, new_local)
```

```python
import jax
import jax.numpy as jnp
from jax import lax
from jax.experimental import pallas as pl
from jax.experimental.pallas import tpu as pltpu
from jax.sharding import Mesh, PartitionSpec as P

HD = 256

norm_eps = 1e-06
outer_rate = 0.7
outer_beta = 0.9
inner_rate = 0.1


PLANE = ("y", "x", "c")
OWNERS = ("zh", "y", "x", "c")
F32 = jnp.float32
BF16 = jnp.bfloat16


def plane_shift(value, hops, first):
    pairs = []
    for y in range(4):
        for x in range(4):
            for c in range(2):
                along_x = (c == 0) == first
                ny, nx = (y, (x + hops) % 4) if along_x else ((y + hops) % 4, x)
                pairs.append(((y * 4 + x) * 2 + c, (ny * 4 + nx) * 2 + c))
    return lax.ppermute(value, PLANE, pairs)


def swap(value, axis):
    return lax.ppermute(value, axis, [(0, 1), (1, 0)])


def mp_shift(value, hops):
    return lax.ppermute(value, "mp", [(i, (i + hops) % 4) for i in range(4)])


def spec_of(shape):
    zeros = (0,) * len(shape)
    return pl.BlockSpec(shape, lambda *_: zeros)


def call(body, meta, ins, outs, grid=(1,), in_specs=None):
    return pl.pallas_call(
        body,
        grid_spec=pltpu.PrefetchScalarGridSpec(
            num_scalar_prefetch=1,
            grid=grid,
            in_specs=in_specs or [spec_of(v.shape) for v in ins],
            out_specs=[spec_of(s.shape) for s in outs],
        ),
        out_shape=outs,
    )(meta, *ins)


def pair_sums(meta, grads, received, matrix):
    rows, cols = received.shape[1:]

    def block(k, t, j):
        return (j // 4) * 16 + lax.rem(t[1] + k, 4) * t[3] + (j % 4) * t[4]

    def own_spec(j):
        return pl.BlockSpec((1, 1, 1, rows, cols), lambda k, t: (matrix, block(k, t, j), t[0], 0, 0))

    def received_spec(j):
        return pl.BlockSpec((1, rows, cols), lambda k, t: (block(k, t, j), 0, 0))

    def body(t, *refs):
        k = pl.program_id(0)
        for step in range(4):

            @pl.when(k == step)
            def _(step=step):
                for j in range(8):
                    total = refs[j][0, 0, 0].astype(F32) + refs[8 + j][0].astype(F32)
                    refs[16 + step][j] = total.astype(BF16)

    return call(
        body,
        meta,
        [grads] * 8 + [received] * 8,
        [jax.ShapeDtypeStruct((8, rows, cols), BF16)] * 4,
        grid=(4,),
        in_specs=[own_spec(j) for j in range(8)] + [received_spec(j) for j in range(8)],
    )


def line_sums(meta, parts):
    rows, cols = parts[0].shape[1:]

    def body(t, *refs):
        for k in range(4):
            at = lax.rem(t[2] + k, 4)
            for z in range(2):
                total = refs[0][z * 4 + at].astype(F32)
                for i in range(1, 4):
                    total = total + refs[i][z * 4 + at].astype(F32)
                refs[4 + k][z] = total.astype(refs[4 + k].dtype)

    return call(
        body,
        meta,
        parts,
        [jax.ShapeDtypeStruct((2, rows, cols), F32 if k == 0 else BF16) for k in range(4)],
    )


def last_sums(meta, parts):
    rows, cols = parts[0].shape[1:]

    def body(t, *refs):
        for k in range(2):
            at = t[5] if k == 0 else 1 - t[5]
            total = refs[0][at]
            for i in range(1, 4):
                total = total + refs[i][at].astype(F32)
            refs[4 + k][...] = total.astype(refs[4 + k].dtype)

    return call(
        body,
        meta,
        parts,
        [jax.ShapeDtypeStruct((rows, cols), F32), jax.ShapeDtypeStruct((rows, cols), BF16)],
    )


def line_rows(meta, parts):
    rows, cols = parts[0].shape[1:]

    def body(t, *refs):
        for k in range(4):
            at = lax.rem(t[2] + 4 - k, 4)
            for z in range(2):
                refs[4][z * 4 + at] = refs[k][z]

    return call(body, meta, parts, [jax.ShapeDtypeStruct((8, rows, cols), BF16)])[0]


def all_rows(meta, own, other):
    rows, cols = own[0].shape[1:]

    def body(t, *refs):
        for side in range(2):
            core = t[0] if side == 0 else 1 - t[0]
            start = t[1] if side == 0 else t[2]
            first = t[3] if side == 0 else t[4]
            second = t[4] if side == 0 else t[3]
            for k in range(4):
                a = lax.rem(start + 4 - k, 4)
                for z in range(2):
                    for b in range(4):
                        at = (z * 16 + a * first + b * second) * 2 + core
                        refs[8][at] = refs[side * 4 + k][z * 4 + b]

    return call(body, meta, own + other, [jax.ShapeDtypeStruct((64, rows, cols), BF16)])[0]


def split_up(value, dim, length):
    before, after = (value.shape[:dim], value.shape[dim + 1 :])
    return jnp.moveaxis(value.reshape(*before, length, -1, *after), dim, 0)


def sum_at_owner(value, axis, dim):
    length = lax.axis_size(axis)
    tiles = lax.all_to_all(split_up(value, dim, length), axis, 0, 0, tiled=True)
    return jnp.sum(tiles.astype(F32), axis=0)


def gathered(value, here):
    rows, width = value.shape
    whole = jnp.zeros((rows, 4 * width), value.dtype)
    for hops in range(4):
        part = value if hops == 0 else mp_shift(value, hops)
        whole = lax.dynamic_update_slice(whole, part, (0, lax.rem(here + 4 - hops, 4) * width))
    return whole


def shards(pseudo_grad, outer_params, momentum, acts, queries, keys, doc_ids):
    workers = lax.axis_size(OWNERS)
    groups = lax.axis_size("mp")
    here = lax.axis_index("mp")
    zh, y, x, c = (lax.axis_index(name) for name in OWNERS)
    first, second = (jnp.where(c == 0, x, y), jnp.where(c == 0, y, x))
    meta = jnp.stack([c, first, second, 1 + 3 * c, 4 - 3 * c, zh]).astype(jnp.int32)
    matrices, rows, cols = outer_params.shape

    grads = pseudo_grad.reshape(matrices, workers // 2, 2, rows, cols)
    received = [
        swap(lax.dynamic_index_in_dim(grads[m], 1 - c, axis=1, keepdims=False), "c")
        for m in range(matrices)
    ]
    full_x = gathered(acts, here)
    count, width = full_x.shape

    weights, new_outer, new_momentum = [], [], []
    for m in range(matrices):
        mine, *sends = pair_sums(meta, grads, received[m], m)
        parts = [mine] + [plane_shift(sends[k - 1], k, True) for k in (1, 2, 3)]
        mine, *sends = line_sums(meta, parts)
        parts = [mine] + [plane_shift(sends[k - 1], k, False) for k in (1, 2, 3)]
        mine, send = last_sums(meta, parts)
        delta = (mine + swap(send, "zh").astype(F32)) / workers
        moment_next = outer_beta * momentum[m] + delta
        params_next = outer_params[m] - outer_rate * (delta + outer_beta * moment_next)
        new_outer.append(params_next)
        new_momentum.append(moment_next)
        piece = params_next.astype(BF16)
        far = swap(piece, "zh")
        both = jnp.stack([jnp.where(zh == 0, piece, far), jnp.where(zh == 0, far, piece)])
        line = line_rows(meta, [both] + [plane_shift(both, k, False) for k in (1, 2, 3)])
        own = [line] + [plane_shift(line, k, True) for k in (1, 2, 3)]
        other = [swap(part, "c") for part in own]
        weights.append(all_rows(meta, own, other).reshape(width, cols))

    heads_here = cols // HD
    all_cols = cols * groups
    rows_f = full_x.astype(F32)
    normed = (
        rows_f * lax.rsqrt(jnp.mean(rows_f * rows_f, axis=-1, keepdims=True) + norm_eps)
    ).astype(BF16)
    gram = lax.dot_general(normed, normed, (((1,), (1,)), ((), ())), preferred_element_type=F32)

    query = queries.reshape(count, heads_here, HD)
    keyed = keys.reshape(count, heads_here, HD)
    scores = jnp.einsum("qhd,khd->hqk", query, keyed, preferred_element_type=F32) * HD ** (-0.5)
    row_pos = lax.broadcasted_iota(jnp.int32, (count, count), 0)
    col_pos = lax.broadcasted_iota(jnp.int32, (count, count), 1)
    allowed = (row_pos >= col_pos) & (doc_ids[:, None] == doc_ids[None, :])
    probs = jax.nn.softmax(jnp.where(allowed[None], scores, -1e30), axis=-1).astype(BF16)

    values = (jnp.dot(normed, weights[0], preferred_element_type=F32) * width ** (-0.5)).astype(BF16)
    context = jnp.einsum(
        "hqk,khd->qhd", probs, values.reshape(count, heads_here, HD), preferred_element_type=F32
    )
    ctx = context.astype(BF16).reshape(count, cols)
    partial_branch = lax.dot_general(
        ctx, weights[1], (((1,), (1,)), ((), ())), preferred_element_type=F32
    ) * all_cols ** (-0.5)
    branch_part = sum_at_owner(partial_branch.astype(BF16), "mp", 1)
    acts_f = acts.astype(F32)
    dout_part = acts_f + branch_part - jnp.roll(acts_f, -1, axis=0)
    dout = lax.all_gather(dout_part.astype(BF16), "mp", axis=1, tiled=True)
    dctx = (jnp.dot(dout, weights[1], preferred_element_type=F32) * all_cols ** (-0.5)).astype(BF16)
    pulled = (
        jnp.einsum(
            "hqk,qhd->khd", probs, dctx.reshape(count, heads_here, HD), preferred_element_type=F32
        )
        .astype(BF16)
        .reshape(count, cols)
    )
    pulled_gram = lax.dot_general(
        pulled, pulled, (((1,), (1,)), ((), ())), preferred_element_type=F32
    )
    squares = jnp.full((8, 128), jnp.sum(gram * pulled_gram) / width)
    squares = squares + lax.ppermute(squares, "mp", [(0, 2), (1, 3), (2, 0), (3, 1)])
    squares = squares + lax.ppermute(squares, "mp", [(0, 1), (1, 0), (2, 3), (3, 2)])
    rms = jnp.sqrt(squares[0, 0] / (width * all_cols) + norm_eps)
    grad = lax.dot_general(
        normed, pulled, (((0,), (0,)), ((), ())), preferred_element_type=F32
    ) * width ** (-0.5)
    new_local = (weights[0].astype(F32) - inner_rate * grad / rms).astype(BF16)
    return (jnp.stack(new_outer), jnp.stack(new_momentum), new_local[None])


def solution(mesh):
    fine = Mesh(mesh.devices.reshape(2, 4, 4, 2, 4), (*OWNERS, "mp"))
    placed = (
        P(OWNERS, None, None, "mp"),
        P(None, OWNERS, "mp"),
        P(None, OWNERS, "mp"),
        P(OWNERS, "mp"),
        P(OWNERS, "mp"),
        P(OWNERS, "mp"),
        P(OWNERS),
    )
    return jax.shard_map(
        shards,
        mesh=fine,
        in_specs=placed,
        out_specs=(P(None, OWNERS, "mp"), P(None, OWNERS, "mp"), P(OWNERS, None, "mp")),
        check_vma=False,
    )
```

```python
import jax
import jax.numpy as jnp
from jax import lax
from jax.experimental import pallas as pl
from jax.experimental.pallas import tpu as pltpu
from jax.sharding import Mesh, PartitionSpec as P

HD = 256

norm_eps = 1e-06
outer_rate = 0.7
outer_beta = 0.9
inner_rate = 0.1


PLANE = ("y", "x", "c")
OWNERS = ("zh", "y", "x", "c")
F32 = jnp.float32
BF16 = jnp.bfloat16


def plane_shift(value, hops, first):
    pairs = []
    for y in range(4):
        for x in range(4):
            for c in range(2):
                along_x = (c == 0) == first
                ny, nx = (y, (x + hops) % 4) if along_x else ((y + hops) % 4, x)
                pairs.append(((y * 4 + x) * 2 + c, (ny * 4 + nx) * 2 + c))
    return lax.ppermute(value, PLANE, pairs)


def swap(value, axis):
    return lax.ppermute(value, axis, [(0, 1), (1, 0)])


def mp_shift(value, hops):
    return lax.ppermute(value, "mp", [(i, (i + hops) % 4) for i in range(4)])


def at(value, axis, index):
    return lax.dynamic_index_in_dim(value, index, axis, keepdims=False)


def all_rows(own, other, pieces):
    rows, cols = own[0].shape[2:]
    part = None if pieces is None else 2 * rows // pieces

    def body(*refs):
        zh, y, x, c = (lax.axis_index(name) for name in OWNERS)
        for side in range(2):
            core = c if side == 0 else 1 - c
            first = jnp.where(core == 0, x, y)
            second = jnp.where(core == 0, y, x)
            for k in range(4):
                a = lax.rem(first + 4 - k, 4) * (1 + 3 * core)
                for j in range(4):
                    b = lax.rem(second + 4 - j, 4) * (4 - 3 * core)
                    owner = (a + b) * 2 + core
                    for z in range(2):
                        value = refs[side * 4 + k][j, z]
                        if pieces is None:
                            far = zh if z == 0 else 1 - zh
                            refs[8][far * 32 + owner] = value
                        else:
                            for half in range(rows // part):
                                q = z * (rows // part) + half
                                refs[8][q, owner] = value[half * part : (half + 1) * part]

    shape = (64, rows, cols) if pieces is None else (pieces, 32, part, cols)
    return pl.pallas_call(
        body,
        in_specs=[pl.BlockSpec(memory_space=pltpu.VMEM)] * 8,
        out_specs=pl.BlockSpec(memory_space=pltpu.VMEM),
        out_shape=jax.ShapeDtypeStruct(shape, BF16),
        compiler_params=pltpu.CompilerParams(vmem_limit_bytes=12 * 2**20),
    )(*own, *other)


def shards(pseudo_grad, outer_params, momentum, acts, queries, keys, doc_ids):
    workers = lax.axis_size(OWNERS)
    groups = lax.axis_size("mp")
    here = lax.axis_index("mp")
    zh, y, x, c = (lax.axis_index(name) for name in OWNERS)
    second = jnp.where(c == 0, y, x)
    matrices, rows, cols = outer_params.shape
    grads = pseudo_grad.reshape(matrices, 2, 4, 4, 2, rows, cols)

    def toward(value, hops):
        return jnp.where(c == 0, at(value, 2, lax.rem(x + hops, 4)), at(value, 1, lax.rem(y + hops, 4)))

    def side(m, core):
        return lax.dynamic_slice(
            grads, (m, 0, 0, 0, core, 0, 0), (1, 2, 4, 4, 1, rows, cols)
        ).reshape(2, 4, 4, rows, cols)

    received = [swap(side(m, 1 - c), "c") for m in range(matrices)]

    full_x = jnp.zeros((acts.shape[0], groups * acts.shape[1]), BF16)
    for hops in range(groups):
        part = acts if hops == 0 else mp_shift(acts, hops)
        full_x = lax.dynamic_update_slice(full_x, part, (0, lax.rem(here + 4 - hops, 4) * acts.shape[1]))
    count, width = full_x.shape

    weights, new_outer, new_momentum = [], [], []
    for m in range(matrices):
        mine = side(m, c)
        sums = [toward(mine, k).astype(F32) + toward(received[m], k).astype(F32) for k in range(4)]
        parts = [lax.optimization_barrier(sums[0].astype(BF16))]
        parts += [plane_shift(sums[k].astype(BF16), k, True) for k in (1, 2, 3)]
        sums = [
            sum(at(part, 1, lax.rem(second + k, 4)).astype(F32) for part in parts) for k in range(4)
        ]
        parts = [lax.optimization_barrier(sums[0])]
        parts += [plane_shift(sums[k].astype(BF16), k, False) for k in (1, 2, 3)]
        send = sum(at(part, 0, 1 - zh).astype(F32) for part in parts).astype(BF16)
        mine = sum(at(part, 0, zh).astype(F32) for part in parts)
        delta = (mine + swap(send, "zh").astype(F32)) / workers
        moment_next = outer_beta * momentum[m] + delta
        params_next = outer_params[m] - outer_rate * (delta + outer_beta * moment_next)
        new_outer.append(params_next)
        new_momentum.append(moment_next)
        piece = params_next.astype(BF16)
        both = jnp.stack([piece, swap(piece, "zh")])
        if m == 1:
            quarters = both.reshape(groups, 2 * rows // groups, cols)
            taken = [at(quarters, 0, lax.rem(here + k, 4)) for k in range(groups)]
            taken = [taken[0]] + [mp_shift(taken[k], k) for k in range(1, groups)]
            both = jnp.stack(taken).reshape(both.shape)
        line = jnp.stack([both] + [plane_shift(both, k, False) for k in (1, 2, 3)])
        own = [line] + [plane_shift(line, k, True) for k in (1, 2, 3)]
        other = [swap(part, "c") for part in own]
        weights.append(all_rows(own, other, None if m == 0 else groups))
    value_proj = weights[0].reshape(width, cols)
    out_proj = weights[1].reshape(groups, width // groups, cols)

    heads_here = cols // HD
    all_cols = cols * groups
    rows_f = full_x.astype(F32)
    normed = (
        rows_f * lax.rsqrt(jnp.mean(rows_f * rows_f, axis=-1, keepdims=True) + norm_eps)
    ).astype(BF16)
    gram = lax.dot_general(normed, normed, (((1,), (1,)), ((), ())), preferred_element_type=F32)
    half = lax.dynamic_slice(full_x, (0, (zh ^ (here // 2)) * (width // 2)), (count, width // 2))
    part = 2 * rows // groups
    row_at = lax.broadcasted_iota(jnp.int32, (width // 2, width // groups), 0)
    col_at = lax.broadcasted_iota(jnp.int32, (width // 2, width // groups), 1)
    pick = row_at == (col_at // part) * rows + (here % 2) * part + col_at % part
    acts_here = jnp.dot(half, pick.astype(BF16), preferred_element_type=F32)

    query = queries.reshape(count, heads_here, HD)
    keyed = keys.reshape(count, heads_here, HD)
    scores = jnp.einsum("qhd,khd->hqk", query, keyed, preferred_element_type=F32) * HD ** (-0.5)
    row_pos = lax.broadcasted_iota(jnp.int32, (count, count), 0)
    col_pos = lax.broadcasted_iota(jnp.int32, (count, count), 1)
    allowed = (row_pos >= col_pos) & (doc_ids[:, None] == doc_ids[None, :])
    probs = jax.nn.softmax(jnp.where(allowed[None], scores, -1e30), axis=-1).astype(BF16)

    values = (jnp.dot(normed, value_proj, preferred_element_type=F32) * width ** (-0.5)).astype(BF16)
    context = jnp.einsum(
        "hqk,khd->qhd", probs, values.reshape(count, heads_here, HD), preferred_element_type=F32
    )
    ctx = context.astype(BF16).reshape(count, cols)
    branch = jnp.zeros((count, width // groups), F32)
    for hops in range(groups):
        part = ctx if hops == 0 else mp_shift(ctx, hops)
        branch = branch + lax.dot_general(
            part, out_proj[hops], (((1,), (1,)), ((), ())), preferred_element_type=F32
        )
    branch = branch * all_cols ** (-0.5)
    dout = (acts_here + branch - jnp.roll(acts_here, -1, axis=0)).astype(BF16)
    dctx = 0.0
    for hops in (1, 2, 3, 0):
        part = jnp.dot(dout, out_proj[hops], preferred_element_type=F32) * all_cols ** (-0.5)
        dctx = dctx + (part if hops == 0 else mp_shift(part.astype(BF16), 4 - hops).astype(F32))
    dctx = dctx.astype(BF16)
    pulled = (
        jnp.einsum(
            "hqk,qhd->khd", probs, dctx.reshape(count, heads_here, HD), preferred_element_type=F32
        )
        .astype(BF16)
        .reshape(count, cols)
    )
    pulled_gram = lax.dot_general(
        pulled, pulled, (((1,), (1,)), ((), ())), preferred_element_type=F32
    )
    squares = jnp.full((8, 128), jnp.sum(gram * pulled_gram) / width)
    squares = squares + lax.ppermute(squares, "mp", [(0, 2), (1, 3), (2, 0), (3, 1)])
    squares = squares + lax.ppermute(squares, "mp", [(0, 1), (1, 0), (2, 3), (3, 2)])
    rms = jnp.sqrt(squares[0, 0] / (width * all_cols) + norm_eps)
    grad = lax.dot_general(
        normed, pulled, (((0,), (0,)), ((), ())), preferred_element_type=F32
    ) * width ** (-0.5)
    new_local = (value_proj.astype(F32) - inner_rate * grad / rms).astype(BF16)
    return (jnp.stack(new_outer), jnp.stack(new_momentum), new_local[None])


def solution(mesh):
    fine = Mesh(mesh.devices.reshape(2, 4, 4, 2, 4), (*OWNERS, "mp"))
    placed = (
        P(OWNERS, None, None, "mp"),
        P(None, OWNERS, "mp"),
        P(None, OWNERS, "mp"),
        P(OWNERS, "mp"),
        P(OWNERS, "mp"),
        P(OWNERS, "mp"),
        P(OWNERS),
    )
    return jax.shard_map(
        shards,
        mesh=fine,
        in_specs=placed,
        out_specs=(P(None, OWNERS, "mp"), P(None, OWNERS, "mp"), P(OWNERS, None, "mp")),
        check_vma=False,
    )
```

```python
import jax
import jax.numpy as jnp
from jax import lax
from jax.experimental import pallas as pl
from jax.experimental.pallas import tpu as pltpu
from jax.sharding import Mesh, PartitionSpec as P

HD = 256

norm_eps = 1e-06
outer_rate = 0.7
outer_beta = 0.9
inner_rate = 0.1


PLANE = ("y", "x", "c")
OWNERS = ("zh", "y", "x", "c")
F32 = jnp.float32
BF16 = jnp.bfloat16
NEAR = (1, 3)


def place(n, near):
    gray = n ^ (n >> 1)
    return gray if near == 3 else (3 * gray) & 3


def plane_swap(value, mask, first):
    pairs = []
    for y in range(4):
        for x in range(4):
            for c in range(2):
                along_x = (c == 0) == first
                ny, nx = (y, x ^ mask) if along_x else (y ^ mask, x)
                pairs.append(((y * 4 + x) * 2 + c, (ny * 4 + nx) * 2 + c))
    return lax.ppermute(value, PLANE, pairs)


def swap(value, axis):
    return lax.ppermute(value, axis, [(0, 1), (1, 0)])


def mp_swap(value, mask):
    return lax.ppermute(value, "mp", [(i, i ^ mask) for i in range(4)])


def local(body, ins, outs, mib, scratch=()):
    spec = pl.BlockSpec(memory_space=pltpu.VMEM)
    return pl.pallas_call(
        body,
        in_specs=[spec] * len(ins),
        out_specs=[spec] * len(outs),
        out_shape=[jax.ShapeDtypeStruct(shape, dtype) for shape, dtype in outs],
        scratch_shapes=scratch,
        compiler_params=pltpu.CompilerParams(vmem_limit_bytes=mib * 2**20),
    )(*ins)


def owner_of(core, first, second):
    return jnp.where(core == 0, second * 4 + first, first * 4 + second)


def pair_sums(grads, received, m):
    rows, cols = received.shape[1:]

    def body(grads_ref, received_ref, *outs):
        zh, y, x, c = (lax.axis_index(name) for name in OWNERS)
        first, second = jnp.where(c == 0, x, y), jnp.where(c == 0, y, x)
        for half in range(2):

            def step(n, carry, half=half):
                i, j, z = n >> 3, (n >> 1) & 3, n & 1
                chip = owner_of(c, first ^ place(2 * half + i, NEAR[m]), second ^ place(j, 3))
                chip = chip + (zh ^ z) * 16
                total = grads_ref[m, chip, c].astype(F32) + received_ref[chip].astype(F32)
                outs[half][i, j, z] = total.astype(BF16)
                return carry

            lax.fori_loop(0, 16, step, 0)

    return local(body, [grads, received], [((2, 4, 2, rows, cols), BF16)] * 2, 20)


def all_rows(parts, m, pieces):
    rows, cols = parts[0].shape[3:]
    part = 2 * rows // pieces

    def body(*refs):
        zh, y, x, c = (lax.axis_index(name) for name in OWNERS)
        for source in range(4):
            core = c if source < 2 else 1 - c
            first, second = jnp.where(core == 0, x, y), jnp.where(core == 0, y, x)

            def step(n, carry, source=source, core=core, first=first, second=second):
                i, j, z = n >> 3, (n >> 1) & 3, n & 1
                chip = owner_of(
                    core, first ^ place(2 * (source % 2) + i, NEAR[m]), second ^ place(j, 3)
                )
                value = refs[source][i, j, z]
                if m == 0:
                    refs[4][(zh ^ z) * 32 + chip * 2 + core] = value
                else:
                    for h in range(rows // part):
                        at = z * (rows // part) + h
                        refs[4][at, chip * 2 + core] = value[h * part : (h + 1) * part]
                return carry

            lax.fori_loop(0, 16, step, 0)

    shape = (64, rows, cols) if m == 0 else (pieces, 32, part, cols)
    return local(body, parts, [(shape, BF16)], 16)[0]


def dot(a, b, a_dim=1, b_dim=0):
    return lax.dot_general(a, b, (((a_dim,), (b_dim,)), ((), ())), preferred_element_type=F32)


def prepare(acts_parts, queries, keys, docs_row, docs_col):
    count, width = acts_parts[0].shape
    heads = queries.shape[1] // HD

    def body(*refs):
        query_ref, key_ref, row_ref, col_ref = refs[4:8]
        full_ref, normed_ref, turned_ref, gram_ref, probs_ref = refs[8:]
        here = lax.axis_index("mp")
        for k in range(4):
            full_ref[:, pl.ds(pl.multiple_of((here ^ k) * width, 128), width)] = refs[k][...]
        rows_f = full_ref[...].astype(F32)
        mean = jnp.mean(rows_f * rows_f, axis=-1, keepdims=True)
        normed = (rows_f * lax.rsqrt(mean + norm_eps)).astype(BF16)
        normed_ref[...] = normed
        turned_ref[...] = jnp.transpose(normed.astype(F32)).astype(BF16)
        gram_ref[...] = dot(normed, normed, 1, 1)
        row_pos = lax.broadcasted_iota(jnp.int32, (count, count), 0)
        col_pos = lax.broadcasted_iota(jnp.int32, (count, count), 1)
        allowed = (row_pos >= col_pos) & (row_ref[...] == col_ref[...])
        for h in range(heads):
            span = slice(h * HD, (h + 1) * HD)
            scores = dot(query_ref[:, span], key_ref[:, span], 1, 1) * HD ** (-0.5)
            scores = jnp.where(allowed, scores, -1e30)
            raised = jnp.exp(scores - jnp.max(scores, axis=-1, keepdims=True))
            probs_ref[h] = (raised / jnp.sum(raised, axis=-1, keepdims=True)).astype(BF16)

    outs = [
        ((count, 4 * width), BF16),
        ((count, 4 * width), BF16),
        ((4 * width, count), BF16),
        ((count, count), F32),
        ((heads, count, count), BF16),
    ]
    return local(body, [*acts_parts, queries, keys, docs_row, docs_col], outs, 16)


def attend(normed, value_proj, probs):
    count, width = normed.shape
    cols = value_proj.shape[1]

    def body(normed_ref, proj_ref, probs_ref, ctx_ref):
        values = (dot(normed_ref[...], proj_ref[...]) * width ** (-0.5)).astype(BF16)
        for h in range(cols // HD):
            span = slice(h * HD, (h + 1) * HD)
            ctx_ref[:, span] = dot(probs_ref[h], values[:, span]).astype(BF16)

    return local(body, [normed, value_proj, probs], [((count, cols), BF16)], 16)[0]


def first_branch(parts, out_proj):
    shape = (parts[0].shape[0], out_proj.shape[1])

    def body(*refs):
        total = dot(refs[0][...], refs[-2][0], 1, 1)
        for k in range(1, len(parts)):
            total = total + dot(refs[k][...], refs[-2][k], 1, 1)
        refs[-1][...] = total

    return local(body, [*parts, out_proj], [(shape, F32)], 16)[0]


def output_grad(branch, last, out_proj, moved):
    count, cols = last.shape
    scale = (4 * cols) ** (-0.5)

    def body(branch_ref, last_ref, proj_ref, moved_ref, *outs):
        total = (branch_ref[...] + dot(last_ref[...], proj_ref[3], 1, 1)) * scale
        dout = (moved_ref[...] + total).astype(BF16)
        for k in range(4):
            outs[k][...] = (dot(dout, proj_ref[k]) * scale).astype(outs[k].dtype)

    return local(
        body,
        [branch, last, out_proj, moved],
        [((count, cols), F32 if k == 0 else BF16) for k in range(4)],
        16,
    )


def values_grad(parts, probs, gram, width):
    count, cols = parts[0].shape

    def body(*refs):
        probs_ref, gram_ref, pulled_ref, squares_ref = refs[4:]
        total = refs[0][...]
        for k in range(1, 4):
            total = total + refs[k][...].astype(F32)
        dctx = total.astype(BF16)
        pulled = jnp.concatenate(
            [
                dot(probs_ref[h], dctx[:, h * HD : (h + 1) * HD], 0, 0).astype(BF16)
                for h in range(cols // HD)
            ],
            axis=1,
        )
        pulled_ref[...] = pulled
        product = gram_ref[...] * dot(pulled, pulled, 1, 1)
        total = jnp.sum(jnp.sum(product, axis=1, keepdims=True), axis=0, keepdims=True)
        squares_ref[...] = jnp.broadcast_to(total / width, (8, 128))

    return local(
        body, [*parts, probs, gram], [((count, cols), BF16), ((8, 128), F32)], 8
    )


def inner_update(turned, pulled, value_proj, squares, entries):
    width, count = turned.shape
    cols = pulled.shape[1]
    block = 512

    def body(turned_ref, pulled_ref, proj_ref, squares_ref, out_ref):
        rms = jnp.sqrt(squares_ref[0:1, 0:1] / entries + norm_eps)
        grad = dot(turned_ref[...], pulled_ref[...])
        out_ref[...] = (proj_ref[...].astype(F32) - grad * (inner_rate * width ** (-0.5) / rms)).astype(
            BF16
        )

    return pl.pallas_call(
        body,
        grid=(width // block,),
        in_specs=[
            pl.BlockSpec((block, count), lambda i: (i, 0)),
            pl.BlockSpec((count, cols), lambda i: (0, 0)),
            pl.BlockSpec((block, cols), lambda i: (i, 0)),
            pl.BlockSpec((8, 128), lambda i: (0, 0)),
        ],
        out_specs=pl.BlockSpec((block, cols), lambda i: (i, 0)),
        out_shape=jax.ShapeDtypeStruct((width, cols), BF16),
        compiler_params=pltpu.CompilerParams(vmem_limit_bytes=12 * 2**20),
    )(turned, pulled, value_proj, squares)


def shards(pseudo_grad, outer_params, momentum, acts, queries, keys, doc_ids):
    workers = lax.axis_size(OWNERS)
    groups = lax.axis_size("mp")
    here = lax.axis_index("mp")
    zh, c = lax.axis_index("zh"), lax.axis_index("c")
    matrices, rows, cols = outer_params.shape
    grads = pseudo_grad.reshape(matrices, 32, 2, rows, cols)

    received = [
        swap(
            lax.dynamic_slice(grads, (m, 0, 1 - c, 0, 0), (1, 32, 1, rows, cols)).reshape(
                32, rows, cols
            ),
            "c",
        )
        for m in range(matrices)
    ]
    kept = []
    for m in range(matrices):
        keep, send = pair_sums(grads, received[m], m)
        if m == 1:
            acts, send = lax.optimization_barrier((acts, send))
        got = plane_swap(send, NEAR[m], True)
        total = keep.astype(F32) + got.astype(F32)
        kept.append(total[0] + plane_swap(total[1].astype(BF16), NEAR[m] ^ 2, True).astype(F32))
    acts_parts = [acts] + [mp_swap(acts, k) for k in (1, 2, 3)]

    send = jnp.stack([value[2:] for value in kept]).astype(BF16)
    total = jnp.stack([value[:2] for value in kept]) + plane_swap(send, 3, False).astype(F32)
    total = total[:, 0] + plane_swap(total[:, 1].astype(BF16), 1, False).astype(F32)
    total = total[:, 0] + swap(total[:, 1].astype(BF16), "zh").astype(F32)

    delta = total / workers
    new_momentum = outer_beta * momentum + delta
    new_outer = outer_params - outer_rate * (delta + outer_beta * new_momentum)

    weights = new_outer.astype(BF16)
    far = swap(weights, "zh")
    gathered = []
    for m in range(matrices):
        both = jnp.stack([weights[m], far[m]])
        if m == 1:
            quarters = both.reshape(groups, 2 * rows // groups, cols)
            taken = [
                lax.dynamic_index_in_dim(quarters, here ^ k, 0, keepdims=False)
                for k in range(groups)
            ]
            taken = [taken[0]] + [mp_swap(taken[k], k) for k in range(1, groups)]
            both = jnp.stack(taken).reshape(both.shape)
        two = jnp.stack([both, plane_swap(both, 1, False)])
        line = jnp.concatenate([two, plane_swap(two, 3, False)])
        two = jnp.stack([line, plane_swap(line, NEAR[m] ^ 2, True)])
        others = plane_swap(two, NEAR[m], True)
        parts = [two, others, swap(two, "c"), swap(others, "c")]
        gathered.append(all_rows(parts, m, groups))
    width = 64 * rows
    value_proj = gathered[0].reshape(width, cols)
    out_proj = gathered[1].reshape(groups, width // groups, cols)

    full_x, normed, turned, gram, probs = prepare(
        acts_parts, queries, keys, doc_ids.reshape(1, -1), doc_ids.reshape(-1, 1)
    )
    count = full_x.shape[0]
    half = lax.dynamic_slice(full_x, (0, (zh ^ (here >> 1)) * (width // 2)), (count, width // 2))
    part = 2 * rows // groups
    row_at = lax.broadcasted_iota(jnp.int32, (width // 2, width // groups), 0)
    col_at = lax.broadcasted_iota(jnp.int32, (width // 2, width // groups), 1)
    pick = row_at == (col_at // part) * rows + (here & 1) * part + col_at % part
    acts_here = dot(half, pick.astype(BF16))
    moved = acts_here - jnp.roll(acts_here, -1, axis=0)

    ctx = attend(normed, value_proj, probs)
    ctx_parts = [mp_swap(ctx, k) for k in (3, 2, 1)][::-1]
    branch = first_branch([ctx, *ctx_parts[:2]], out_proj)
    mine, *sends = output_grad(branch, ctx_parts[2], out_proj, moved)
    dctx_parts = [mine] + [mp_swap(sends[k - 1], k) for k in (3, 2, 1)]
    pulled, squares = values_grad(dctx_parts, probs, gram, width)
    squares = squares + mp_swap(squares, 2)
    squares = squares + mp_swap(squares, 1)
    new_local = inner_update(turned, pulled, value_proj, squares, width * cols * groups)
    return (new_outer, new_momentum, new_local[None])


def solution(mesh):
    fine = Mesh(mesh.devices.reshape(2, 4, 4, 2, 4), (*OWNERS, "mp"))
    placed = (
        P(OWNERS, None, None, "mp"),
        P(None, OWNERS, "mp"),
        P(None, OWNERS, "mp"),
        P(OWNERS, "mp"),
        P(OWNERS, "mp"),
        P(OWNERS, "mp"),
        P(OWNERS),
    )
    return jax.shard_map(
        shards,
        mesh=fine,
        in_specs=placed,
        out_specs=(P(None, OWNERS, "mp"), P(None, OWNERS, "mp"), P(OWNERS, None, "mp")),
        check_vma=False,
    )
```

```python
import jax
import jax.numpy as jnp
from jax import lax
from jax.experimental import pallas as pl
from jax.experimental.pallas import tpu as pltpu
from jax.sharding import Mesh, PartitionSpec as P


HD = 256

norm_eps = 1e-06
outer_rate = 0.7
outer_beta = 0.9
inner_rate = 0.1


PLANE = ("y", "x", "c")
OWNERS = ("zh", "y", "x", "c")
F32 = jnp.float32
BF16 = jnp.bfloat16
NEAR = (1, 3)


def place(n, near):
    gray = n ^ (n >> 1)
    return gray if near == 3 else (3 * gray) & 3


def plane_swap(value, mask, first):
    pairs = []
    for y in range(4):
        for x in range(4):
            for c in range(2):
                along_x = (c == 0) == first
                ny, nx = (y, x ^ mask) if along_x else (y ^ mask, x)
                pairs.append(((y * 4 + x) * 2 + c, (ny * 4 + nx) * 2 + c))
    return lax.ppermute(value, PLANE, pairs)


def swap(value, axis):
    return lax.ppermute(value, axis, [(0, 1), (1, 0)])


def mp_swap(value, mask):
    return lax.ppermute(value, "mp", [(i, i ^ mask) for i in range(4)])


def local(body, ins, outs, mib, scratch=()):
    spec = pl.BlockSpec(memory_space=pltpu.VMEM)
    return pl.pallas_call(
        body,
        in_specs=[spec] * len(ins),
        out_specs=[spec] * len(outs),
        out_shape=[jax.ShapeDtypeStruct(shape, dtype) for shape, dtype in outs],
        scratch_shapes=scratch,
        compiler_params=pltpu.CompilerParams(vmem_limit_bytes=mib * 2**20),
    )(*ins)


def owner_of(core, first, second):
    return jnp.where(core == 0, second * 4 + first, first * 4 + second)


def pair_sums(grads, received, m):
    rows, cols = received.shape[1:]

    def body(grads_ref, received_ref, *outs):
        zh, y, x, c = (lax.axis_index(name) for name in OWNERS)
        first, second = jnp.where(c == 0, x, y), jnp.where(c == 0, y, x)
        for half in range(2):

            def step(n, carry, half=half):
                i, j, z = n >> 3, (n >> 1) & 3, n & 1
                chip = owner_of(c, first ^ place(2 * half + i, NEAR[m]), second ^ place(j, 3))
                chip = chip + (zh ^ z) * 16
                total = grads_ref[m, chip, c].astype(F32) + received_ref[chip].astype(F32)
                outs[half][i, j, z] = total.astype(BF16)
                return carry

            lax.fori_loop(0, 16, step, 0)

    return local(body, [grads, received], [((2, 4, 2, rows, cols), BF16)] * 2, 20)


def all_rows(parts, m, pieces):
    rows, cols = parts[0].shape[3:]
    part = 2 * rows // pieces

    def body(*refs):
        zh, y, x, c = (lax.axis_index(name) for name in OWNERS)
        for source in range(4):
            core = c if source < 2 else 1 - c
            first, second = jnp.where(core == 0, x, y), jnp.where(core == 0, y, x)

            def step(n, carry, source=source, core=core, first=first, second=second):
                i, j, z = n >> 3, (n >> 1) & 3, n & 1
                chip = owner_of(
                    core, first ^ place(2 * (source % 2) + i, NEAR[m]), second ^ place(j, 3)
                )
                value = refs[source][i, j, z]
                if m == 0:
                    refs[4][(zh ^ z) * 32 + chip * 2 + core] = value
                else:
                    for h in range(rows // part):
                        at = z * (rows // part) + h
                        refs[4][at, chip * 2 + core] = value[h * part : (h + 1) * part]
                return carry

            lax.fori_loop(0, 16, step, 0)

    shape = (64, rows, cols) if m == 0 else (pieces, 32, part, cols)
    return local(body, parts, [(shape, BF16)], 16)[0]


def dot(a, b, a_dim=1, b_dim=0):
    return lax.dot_general(a, b, (((a_dim,), (b_dim,)), ((), ())), preferred_element_type=F32)


def prepare(acts_parts, queries, keys, docs_row, docs_col):
    count, width = acts_parts[0].shape
    heads = queries.shape[1] // HD

    def body(*refs):
        query_ref, key_ref, row_ref, col_ref = refs[4:8]
        full_ref, normed_ref, turned_ref, gram_ref, probs_ref = refs[8:]
        here = lax.axis_index("mp")
        for k in range(4):
            full_ref[:, pl.ds(pl.multiple_of((here ^ k) * width, 128), width)] = refs[k][...]
        rows_f = full_ref[...].astype(F32)
        mean = jnp.mean(rows_f * rows_f, axis=-1, keepdims=True)
        normed = (rows_f * lax.rsqrt(mean + norm_eps)).astype(BF16)
        normed_ref[...] = normed
        turned_ref[...] = jnp.transpose(normed.astype(F32)).astype(BF16)
        gram_ref[...] = dot(normed, normed, 1, 1)
        row_pos = lax.broadcasted_iota(jnp.int32, (count, count), 0)
        col_pos = lax.broadcasted_iota(jnp.int32, (count, count), 1)
        allowed = (row_pos >= col_pos) & (row_ref[...] == col_ref[...])
        for h in range(heads):
            span = slice(h * HD, (h + 1) * HD)
            scores = dot(query_ref[:, span], key_ref[:, span], 1, 1) * HD ** (-0.5)
            scores = jnp.where(allowed, scores, -1e30)
            raised = jnp.exp(scores - jnp.max(scores, axis=-1, keepdims=True))
            probs_ref[h] = (raised / jnp.sum(raised, axis=-1, keepdims=True)).astype(BF16)

    outs = [
        ((count, 4 * width), BF16),
        ((count, 4 * width), BF16),
        ((4 * width, count), BF16),
        ((count, count), F32),
        ((heads, count, count), BF16),
    ]
    return local(body, [*acts_parts, queries, keys, docs_row, docs_col], outs, 16)


def attend(normed, value_proj, probs):
    count, width = normed.shape
    cols = value_proj.shape[1]

    def body(normed_ref, proj_ref, probs_ref, ctx_ref):
        values = (dot(normed_ref[...], proj_ref[...]) * width ** (-0.5)).astype(BF16)
        for h in range(cols // HD):
            span = slice(h * HD, (h + 1) * HD)
            ctx_ref[:, span] = dot(probs_ref[h], values[:, span]).astype(BF16)

    return local(body, [normed, value_proj, probs], [((count, cols), BF16)], 16)[0]


def first_branch(parts, out_proj):
    shape = (parts[0].shape[0], out_proj.shape[1])

    def body(*refs):
        total = dot(refs[0][...], refs[-2][0], 1, 1)
        for k in range(1, len(parts)):
            total = total + dot(refs[k][...], refs[-2][k], 1, 1)
        refs[-1][...] = total

    return local(body, [*parts, out_proj], [(shape, F32)], 16)[0]


def output_grad(branch, last, out_proj, moved):
    count, cols = last.shape
    scale = (4 * cols) ** (-0.5)

    def body(branch_ref, last_ref, proj_ref, moved_ref, *outs):
        total = (branch_ref[...] + dot(last_ref[...], proj_ref[3], 1, 1)) * scale
        dout = (moved_ref[...] + total).astype(BF16)
        for k in range(4):
            outs[k][...] = (dot(dout, proj_ref[k]) * scale).astype(outs[k].dtype)

    return local(
        body,
        [branch, last, out_proj, moved],
        [((count, cols), F32 if k == 0 else BF16) for k in range(4)],
        16,
    )


def values_grad(parts, probs, gram, width):
    count, cols = parts[0].shape

    def body(*refs):
        probs_ref, gram_ref, pulled_ref, squares_ref = refs[4:]
        total = refs[0][...]
        for k in range(1, 4):
            total = total + refs[k][...].astype(F32)
        dctx = total.astype(BF16)
        pulled = jnp.concatenate(
            [
                dot(probs_ref[h], dctx[:, h * HD : (h + 1) * HD], 0, 0).astype(BF16)
                for h in range(cols // HD)
            ],
            axis=1,
        )
        pulled_ref[...] = pulled
        product = gram_ref[...] * dot(pulled, pulled, 1, 1)
        total = jnp.sum(jnp.sum(product, axis=1, keepdims=True), axis=0, keepdims=True)
        squares_ref[...] = jnp.broadcast_to(total / width, (8, 128))

    return local(
        body, [*parts, probs, gram], [((count, cols), BF16), ((8, 128), F32)], 8
    )


def weight_grad(turned, pulled):
    def body(turned_ref, pulled_ref, out_ref):
        out_ref[...] = dot(turned_ref[...], pulled_ref[...])

    return local(body, [turned, pulled], [((turned.shape[0], pulled.shape[1]), F32)], 16)[0]


def inner_update(grad, value_proj, squares, entries):
    width, cols = value_proj.shape
    block = 512

    def body(grad_ref, proj_ref, squares_ref, out_ref):
        rms = jnp.sqrt(squares_ref[0:1, 0:1] / entries + norm_eps)
        scale = inner_rate * width ** (-0.5) / rms
        out_ref[...] = (proj_ref[...].astype(F32) - grad_ref[...] * scale).astype(BF16)

    return pl.pallas_call(
        body,
        grid=(width // block,),
        in_specs=[
            pl.BlockSpec((block, cols), lambda i: (i, 0)),
            pl.BlockSpec((block, cols), lambda i: (i, 0)),
            pl.BlockSpec((8, 128), lambda i: (0, 0)),
        ],
        out_specs=pl.BlockSpec((block, cols), lambda i: (i, 0)),
        out_shape=jax.ShapeDtypeStruct((width, cols), BF16),
        compiler_params=pltpu.CompilerParams(vmem_limit_bytes=12 * 2**20),
    )(grad, value_proj, squares)


def shards(pseudo_grad, outer_params, momentum, acts, queries, keys, doc_ids):
    workers = lax.axis_size(OWNERS)
    groups = lax.axis_size("mp")
    here = lax.axis_index("mp")
    zh, c = lax.axis_index("zh"), lax.axis_index("c")
    matrices, rows, cols = outer_params.shape
    grads = pseudo_grad.reshape(matrices, 32, 2, rows, cols)

    received = [
        swap(
            lax.dynamic_slice(grads, (m, 0, 1 - c, 0, 0), (1, 32, 1, rows, cols)).reshape(
                32, rows, cols
            ),
            "c",
        )
        for m in range(matrices)
    ]
    state = jnp.stack([outer_params, momentum])
    kept = []
    for m in range(matrices):
        keep, send = pair_sums(grads, received[m], m)
        if m == 1:
            acts, state, send = lax.optimization_barrier((acts, state, send))
        got = plane_swap(send, NEAR[m], True)
        total = keep.astype(F32) + got.astype(F32)
        kept.append(total[0] + plane_swap(total[1].astype(BF16), NEAR[m] ^ 2, True).astype(F32))
    acts_parts = [acts] + [mp_swap(acts, k) for k in (1, 2, 3)]
    far_state = swap(state, "zh")
    ready = prepare(acts_parts, queries, keys, doc_ids.reshape(1, -1), doc_ids.reshape(-1, 1))

    send = jnp.stack([value[2:] for value in kept]).astype(BF16)
    got = plane_swap(send, 3, False)
    total = jnp.stack([value[:2] for value in kept]) + got.astype(F32)
    total, ready, far_state = lax.optimization_barrier((total, ready, far_state))
    full_x, normed, turned, gram, probs = ready
    width = 64 * rows
    count = full_x.shape[0]
    half = lax.dynamic_slice(full_x, (0, (zh ^ (here >> 1)) * (width // 2)), (count, width // 2))
    part = 2 * rows // groups
    row_at = lax.broadcasted_iota(jnp.int32, (width // 2, width // groups), 0)
    col_at = lax.broadcasted_iota(jnp.int32, (width // 2, width // groups), 1)
    pick = row_at == (col_at // part) * rows + (here & 1) * part + col_at % part
    acts_here = dot(half, pick.astype(BF16))
    moved = acts_here - jnp.roll(acts_here, -1, axis=0)

    total = total[:, 0] + plane_swap(total[:, 1].astype(BF16), 1, False).astype(F32)
    total = total + swap(total.astype(BF16), "zh").astype(F32)[:, ::-1]
    total, moved = lax.optimization_barrier((total, moved))

    def outer_update(summed, params, moment):
        delta = summed / workers
        moment_next = outer_beta * moment + delta
        return params - outer_rate * (delta + outer_beta * moment_next), moment_next

    new_outer, new_momentum = outer_update(total[:, 0], outer_params, momentum)
    other_outer, _ = outer_update(total[:, 1], far_state[0], far_state[1])
    weights = [
        jnp.stack([new_outer[m].astype(BF16), other_outer[m].astype(BF16)]) for m in range(matrices)
    ]
    gathered = []
    for m in range(matrices):
        both = weights[m]
        if m == 1:
            quarters = both.reshape(groups, 2 * rows // groups, cols)
            taken = [
                lax.dynamic_index_in_dim(quarters, here ^ k, 0, keepdims=False)
                for k in range(groups)
            ]
            taken = [taken[0]] + [mp_swap(taken[k], k) for k in range(1, groups)]
            both = jnp.stack(taken).reshape(both.shape)
        two = jnp.stack([both, plane_swap(both, 1, False)])
        line = jnp.concatenate([two, plane_swap(two, 3, False)])
        two = jnp.stack([line, plane_swap(line, NEAR[m] ^ 2, True)])
        others = plane_swap(two, NEAR[m], True)
        parts = [two, others, swap(two, "c"), swap(others, "c")]
        gathered.append(all_rows(parts, m, groups))
    value_proj = gathered[0].reshape(width, cols)
    out_proj = gathered[1].reshape(groups, width // groups, cols)

    ctx = attend(normed, value_proj, probs)
    ctx_parts = [mp_swap(ctx, k) for k in (3, 2, 1)][::-1]
    branch = first_branch([ctx, *ctx_parts[:2]], out_proj)
    mine, *sends = output_grad(branch, ctx_parts[2], out_proj, moved)
    dctx_parts = [mine] + [mp_swap(sends[k - 1], k) for k in (3, 2, 1)]
    pulled, squares = values_grad(dctx_parts, probs, gram, width)
    grad = weight_grad(turned, pulled)
    squares = squares + mp_swap(squares, 2)
    squares = squares + mp_swap(squares, 1)
    new_local = inner_update(grad, value_proj, squares, width * cols * groups)
    return (new_outer, new_momentum, new_local[None])


def solution(mesh):
    fine = Mesh(mesh.devices.reshape(2, 4, 4, 2, 4), (*OWNERS, "mp"))
    placed = (
        P(OWNERS, None, None, "mp"),
        P(None, OWNERS, "mp"),
        P(None, OWNERS, "mp"),
        P(OWNERS, "mp"),
        P(OWNERS, "mp"),
        P(OWNERS, "mp"),
        P(OWNERS),
    )

    return jax.shard_map(
        shards,
        mesh=fine,
        in_specs=placed,
        out_specs=(P(None, OWNERS, "mp"), P(None, OWNERS, "mp"), P(OWNERS, None, "mp")),
        check_vma=False,
    )
```

```python
import jax
import jax.numpy as jnp
from jax import lax
from jax.experimental import pallas as pl
from jax.experimental.pallas import tpu as pltpu
from jax.sharding import Mesh, PartitionSpec as P


HD = 256

norm_eps = 1e-06
outer_rate = 0.7
outer_beta = 0.9
inner_rate = 0.1


PLANE = ("y", "x", "c")
OWNERS = ("zh", "y", "x", "c")
F32 = jnp.float32
BF16 = jnp.bfloat16
NEAR = (1, 3)
GATHER_NEAR = 1


def place(n, near):
    gray = n ^ (n >> 1)
    return gray if near == 3 else (3 * gray) & 3


def plane_swap(value, mask, first):
    pairs = []
    for y in range(4):
        for x in range(4):
            for c in range(2):
                along_x = (c == 0) == first
                ny, nx = (y, x ^ mask) if along_x else (y ^ mask, x)
                pairs.append(((y * 4 + x) * 2 + c, (ny * 4 + nx) * 2 + c))
    return lax.ppermute(value, PLANE, pairs)


def swap(value, axis):
    return lax.ppermute(value, axis, [(0, 1), (1, 0)])


def mp_swap(value, mask):
    return lax.ppermute(value, "mp", [(i, i ^ mask) for i in range(4)])


def local(body, ins, outs, mib, scratch=()):
    spec = pl.BlockSpec(memory_space=pltpu.VMEM)
    return pl.pallas_call(
        body,
        in_specs=[spec] * len(ins),
        out_specs=[spec] * len(outs),
        out_shape=[jax.ShapeDtypeStruct(shape, dtype) for shape, dtype in outs],
        scratch_shapes=scratch,
        compiler_params=pltpu.CompilerParams(vmem_limit_bytes=mib * 2**20),
    )(*ins)


def owner_of(core, first, second):
    return jnp.where(core == 0, second * 4 + first, first * 4 + second)


def pair_sums(grads, received, m):
    rows, cols = received.shape[1:]

    def body(grads_ref, received_ref, *outs):
        zh, y, x, c = (lax.axis_index(name) for name in OWNERS)
        first, second = jnp.where(c == 0, x, y), jnp.where(c == 0, y, x)
        for half in range(2):

            def step(n, carry, half=half):
                i, j, z = n >> 3, (n >> 1) & 3, n & 1
                chip = owner_of(c, first ^ place(2 * half + i, NEAR[m]), second ^ place(j, 3))
                chip = chip + (zh ^ z) * 16
                total = grads_ref[m, chip, c].astype(F32) + received_ref[chip].astype(F32)
                outs[half][i, j, z] = total.astype(BF16)
                return carry

            lax.fori_loop(0, 16, step, 0)

    return local(body, [grads, received], [((2, 4, 2, rows, cols), BF16)] * 2, 20)


def all_rows(parts, m, pieces):
    rows, cols = parts[0].shape[3:]
    part = 2 * rows // pieces

    def body(*refs):
        zh, y, x, c = (lax.axis_index(name) for name in OWNERS)
        for source in range(4):
            core = c if source < 2 else 1 - c
            first, second = jnp.where(core == 0, x, y), jnp.where(core == 0, y, x)

            def step(n, carry, source=source, core=core, first=first, second=second):
                i, j, z = n >> 3, (n >> 1) & 3, n & 1
                chip = owner_of(
                    core, first ^ place(2 * (source % 2) + i, GATHER_NEAR), second ^ place(j, 3)
                )
                value = refs[source][i, j, z]
                if m == 0:
                    refs[4][(zh ^ z) * 32 + chip * 2 + core] = value
                else:
                    for h in range(rows // part):
                        at = z * (rows // part) + h
                        refs[4][at, chip * 2 + core] = value[h * part : (h + 1) * part]
                return carry

            lax.fori_loop(0, 16, step, 0)

    shape = (64, rows, cols) if m == 0 else (pieces, 32, part, cols)
    return local(body, parts, [(shape, BF16)], 16)[0]


def dot(a, b, a_dim=1, b_dim=0):
    return lax.dot_general(a, b, (((a_dim,), (b_dim,)), ((), ())), preferred_element_type=F32)


def prepare(acts_parts, queries, keys, docs_row, docs_col, rows):
    count, width = acts_parts[0].shape
    heads = queries.shape[1] // HD
    part = rows // 2
    group = 16 * rows

    def body(*refs):
        query_ref, key_ref, row_ref, col_ref = refs[4:8]
        normed_ref, turned_ref, gram_ref, probs_ref, moved_ref, full_ref = refs[8:]
        here, zh = lax.axis_index("mp"), lax.axis_index("zh")
        for k in range(4):
            full_ref[:, pl.ds(pl.multiple_of((here ^ k) * width, 128), width)] = refs[k][...]
        rows_f = full_ref[...].astype(F32)
        mean = jnp.mean(rows_f * rows_f, axis=-1, keepdims=True)
        normed = (rows_f * lax.rsqrt(mean + norm_eps)).astype(BF16)
        normed_ref[...] = normed
        turned_ref[...] = jnp.transpose(normed.astype(F32)).astype(BF16)
        gram_ref[...] = dot(normed, normed, 1, 1)
        row_pos = lax.broadcasted_iota(jnp.int32, (count, count), 0)
        col_pos = lax.broadcasted_iota(jnp.int32, (count, count), 1)
        allowed = (row_pos >= col_pos) & (row_ref[...] == col_ref[...])
        for h in range(heads):
            span = slice(h * HD, (h + 1) * HD)
            scores = dot(query_ref[:, span], key_ref[:, span], 1, 1) * HD ** (-0.5)
            scores = jnp.where(allowed, scores, -1e30)
            raised = jnp.exp(scores - jnp.max(scores, axis=-1, keepdims=True))
            probs_ref[h] = (raised / jnp.sum(raised, axis=-1, keepdims=True)).astype(BF16)
        from_row = lax.broadcasted_iota(jnp.int32, (group, group // 2), 0)
        to_col = lax.broadcasted_iota(jnp.int32, (1, group // 2), 1)
        run = ((to_col.astype(F32) + 0.5) * (1.0 / part)).astype(jnp.int32)
        pick = (from_row == to_col + (run + (here & 1)) * part).astype(F32).astype(BF16)
        for g in range(2):
            start = (zh ^ (here >> 1)) * (2 * width) + g * group
            taken = dot(full_ref[:, pl.ds(pl.multiple_of(start, 128), group)], pick)
            moved = taken - pltpu.roll(taken, count - 1, 0)
            moved_ref[:, g * (group // 2) : (g + 1) * (group // 2)] = moved

    outs = [
        ((count, 4 * width), BF16),
        ((4 * width, count), BF16),
        ((count, count), F32),
        ((heads, count, count), BF16),
        ((count, width), F32),
    ]
    return local(
        body,
        [*acts_parts, queries, keys, docs_row, docs_col],
        outs,
        16,
        [pltpu.VMEM((count, 4 * width), BF16)],
    )


def quarters_of(both):
    rows, cols = both.shape[1:]
    part = rows // 2

    def body(both_ref, *outs):
        here = lax.axis_index("mp")
        for k in range(4):
            value = both_ref[(here ^ k) >> 1]
            odd = ((here ^ k) & 1) == 1
            outs[k][...] = jnp.where(odd, value[part:], value[:part])

    return local(body, [both], [((part, cols), BF16)] * 4, 4)


def attend(normed, value_proj, probs):
    count, width = normed.shape
    cols = value_proj.shape[1]

    def body(normed_ref, proj_ref, probs_ref, ctx_ref):
        values = (dot(normed_ref[...], proj_ref[...]) * width ** (-0.5)).astype(BF16)
        for h in range(cols // HD):
            span = slice(h * HD, (h + 1) * HD)
            ctx_ref[:, span] = dot(probs_ref[h], values[:, span]).astype(BF16)

    return local(body, [normed, value_proj, probs], [((count, cols), BF16)], 16)[0]


def first_branch(parts, out_proj):
    shape = (parts[0].shape[0], out_proj.shape[1])

    def body(*refs):
        total = dot(refs[0][...], refs[-2][0], 1, 1)
        for k in range(1, len(parts)):
            total = total + dot(refs[k][...], refs[-2][k], 1, 1)
        refs[-1][...] = total

    return local(body, [*parts, out_proj], [(shape, F32)], 16)[0]


def output_grad(branch, last, out_proj, moved):
    count, cols = last.shape
    scale = (4 * cols) ** (-0.5)

    def body(branch_ref, last_ref, proj_ref, moved_ref, *outs):
        total = (branch_ref[...] + dot(last_ref[...], proj_ref[3], 1, 1)) * scale
        dout = (moved_ref[...] + total).astype(BF16)
        for k in range(4):
            outs[k][...] = (dot(dout, proj_ref[k]) * scale).astype(outs[k].dtype)

    return local(
        body,
        [branch, last, out_proj, moved],
        [((count, cols), F32 if k == 0 else BF16) for k in range(4)],
        16,
    )


def values_grad(parts, probs, gram, width):
    count, cols = parts[0].shape

    def body(*refs):
        probs_ref, gram_ref, pulled_ref, squares_ref = refs[4:]
        total = refs[0][...]
        for k in range(1, 4):
            total = total + refs[k][...].astype(F32)
        dctx = total.astype(BF16)
        pulled = jnp.concatenate(
            [
                dot(probs_ref[h], dctx[:, h * HD : (h + 1) * HD], 0, 0).astype(BF16)
                for h in range(cols // HD)
            ],
            axis=1,
        )
        pulled_ref[...] = pulled
        product = gram_ref[...] * dot(pulled, pulled, 1, 1)
        total = jnp.sum(jnp.sum(product, axis=1, keepdims=True), axis=0, keepdims=True)
        squares_ref[...] = jnp.broadcast_to(total / width, (8, 128))

    return local(
        body, [*parts, probs, gram], [((count, cols), BF16), ((8, 128), F32)], 8
    )


def weight_grad(turned, pulled):
    def body(turned_ref, pulled_ref, out_ref):
        out_ref[...] = dot(turned_ref[...], pulled_ref[...])

    return local(body, [turned, pulled], [((turned.shape[0], pulled.shape[1]), F32)], 16)[0]


def inner_update(grad, value_proj, squares, entries):
    width, cols = value_proj.shape
    steps = 12
    block = width // steps

    def body(grad_ref, proj_ref, squares_ref, out_ref, held, sems):
        rms = jnp.sqrt(squares_ref[0:1, 0:1] / entries + norm_eps)
        scale = inner_rate * width ** (-0.5) / rms
        copies = []
        for i in range(steps):
            span = pl.ds(i * block, block)
            held[span, :] = (proj_ref[span, :].astype(F32) - grad_ref[span, :] * scale).astype(BF16)
            copies.append(pltpu.make_async_copy(held.at[span, :], out_ref.at[span, :], sems.at[i]))
            copies[-1].start()
        for copy in copies:
            copy.wait()

    vmem = pl.BlockSpec(memory_space=pltpu.VMEM)
    return pl.pallas_call(
        body,
        in_specs=[vmem] * 3,
        out_specs=pl.BlockSpec(memory_space=pl.ANY),
        out_shape=jax.ShapeDtypeStruct((width, cols), BF16),
        scratch_shapes=[pltpu.VMEM((width, cols), BF16), pltpu.SemaphoreType.DMA((steps,))],
        compiler_params=pltpu.CompilerParams(vmem_limit_bytes=20 * 2**20),
    )(grad, value_proj, squares)


def shards(pseudo_grad, outer_params, momentum, acts, queries, keys, doc_ids):
    workers = lax.axis_size(OWNERS)
    groups = lax.axis_size("mp")
    c = lax.axis_index("c")
    matrices, rows, cols = outer_params.shape
    grads = pseudo_grad.reshape(matrices, 32, 2, rows, cols)

    received = [
        swap(
            lax.dynamic_slice(grads, (m, 0, 1 - c, 0, 0), (1, 32, 1, rows, cols)).reshape(
                32, rows, cols
            ),
            "c",
        )
        for m in range(matrices)
    ]
    kept = []
    for m in range(matrices):
        keep, send = pair_sums(grads, received[m], m)
        if m == 1:
            acts, old_outer, old_momentum, send = lax.optimization_barrier(
                (acts, outer_params, momentum, send)
            )
        got = plane_swap(send, NEAR[m], True)
        total = keep.astype(F32) + got.astype(F32)
        got = plane_swap(total[1].astype(BF16), NEAR[m] ^ 2, True)
        kept.append(total[0] + got.astype(F32))
    acts_parts = [acts] + [mp_swap(acts, k) for k in (1, 2, 3)]
    far_state = swap(jnp.stack([old_outer, old_momentum]), "zh")
    normed, turned, gram, probs, moved = prepare(
        acts_parts, queries, keys, doc_ids.reshape(1, -1), doc_ids.reshape(-1, 1), rows
    )

    send = jnp.stack([value[2:] for value in kept]).astype(BF16)
    total = jnp.stack([value[:2] for value in kept]) + plane_swap(send, 3, False).astype(F32)
    total = total[:, 0] + plane_swap(total[:, 1].astype(BF16), 1, False).astype(F32)
    got = swap(total.astype(BF16), "zh")
    total = total + got.astype(F32)[:, ::-1]

    def outer_update(summed, params, moment):
        delta = summed / workers
        moment_next = outer_beta * moment + delta
        return params - outer_rate * (delta + outer_beta * moment_next), moment_next

    new_outer, new_momentum = outer_update(total[:, 0], outer_params, momentum)
    other_outer, _ = outer_update(total[:, 1], far_state[0], far_state[1])
    weights = [
        jnp.stack([new_outer[m].astype(BF16), other_outer[m].astype(BF16)]) for m in range(matrices)
    ]
    gathered = []
    for m in range(matrices):
        both = weights[m]
        if m == 1:
            taken = quarters_of(both)
            taken = [taken[0]] + [mp_swap(taken[k], k) for k in range(1, groups)]
            both = jnp.stack(taken).reshape(both.shape)
        two = jnp.stack([both, plane_swap(both, 1, False)])
        line = jnp.concatenate([two, plane_swap(two, 3, False)])
        two = jnp.stack([line, plane_swap(line, GATHER_NEAR ^ 2, True)])
        others = plane_swap(two, GATHER_NEAR, True)
        near_parts = swap(two, "c")
        parts = [two, others, near_parts, swap(others, "c")]
        gathered.append(all_rows(parts, m, groups))
    width = 64 * rows
    value_proj = gathered[0].reshape(width, cols)
    out_proj = gathered[1].reshape(groups, width // groups, cols)

    ctx = attend(normed, value_proj, probs)
    ctx_parts = []
    for k in (1, 2, 3):
        ctx_parts.append(mp_swap(ctx, k))
    branch = first_branch([ctx, *ctx_parts[:2]], out_proj)
    mine, *sends = output_grad(branch, ctx_parts[2], out_proj, moved)
    dctx_parts = [mine] + [mp_swap(sends[k - 1], k) for k in (3, 2, 1)]
    pulled, squares = values_grad(dctx_parts, probs, gram, width)
    grad = weight_grad(turned, pulled)
    squares = squares + mp_swap(squares, 2)
    squares = squares + mp_swap(squares, 1)
    new_local = inner_update(grad, value_proj, squares, width * cols * groups)
    return (new_outer, new_momentum, new_local[None])


def solution(mesh):
    fine = Mesh(mesh.devices.reshape(2, 4, 4, 2, 4), (*OWNERS, "mp"))
    placed = (
        P(OWNERS, None, None, "mp"),
        P(None, OWNERS, "mp"),
        P(None, OWNERS, "mp"),
        P(OWNERS, "mp"),
        P(OWNERS, "mp"),
        P(OWNERS, "mp"),
        P(OWNERS),
    )

    return jax.shard_map(
        shards,
        mesh=fine,
        in_specs=placed,
        out_specs=(P(None, OWNERS, "mp"), P(None, OWNERS, "mp"), P(OWNERS, None, "mp")),
        check_vma=False,
    )
```

```python
import jax
import jax.numpy as jnp
from jax import lax
from jax.experimental import pallas as pl
from jax.experimental.pallas import tpu as pltpu
from jax.sharding import Mesh, PartitionSpec as P


HD = 256

norm_eps = 1e-06
outer_rate = 0.7
outer_beta = 0.9
inner_rate = 0.1


PLANE = ("y", "x", "c")
OWNERS = ("zh", "y", "x", "c")
F32 = jnp.float32
BF16 = jnp.bfloat16
NEAR = (1, 3)
SECOND_NEAR = (3, 1)


def place(n, near):
    gray = n ^ (n >> 1)
    return gray if near == 3 else (3 * gray) & 3


def plane_swap(value, mask, first):
    pairs = []
    for y in range(4):
        for x in range(4):
            for c in range(2):
                along_x = (c == 0) == first
                ny, nx = (y, x ^ mask) if along_x else (y ^ mask, x)
                pairs.append(((y * 4 + x) * 2 + c, (ny * 4 + nx) * 2 + c))
    return lax.ppermute(value, PLANE, pairs)


def swap(value, axis):
    return lax.ppermute(value, axis, [(0, 1), (1, 0)])


def mp_swap(value, mask):
    return lax.ppermute(value, "mp", [(i, i ^ mask) for i in range(4)])


def local(body, ins, outs, mib, scratch=()):
    spec = pl.BlockSpec(memory_space=pltpu.VMEM)
    return pl.pallas_call(
        body,
        in_specs=[spec] * len(ins),
        out_specs=[spec] * len(outs),
        out_shape=[jax.ShapeDtypeStruct(shape, dtype) for shape, dtype in outs],
        scratch_shapes=scratch,
        compiler_params=pltpu.CompilerParams(vmem_limit_bytes=mib * 2**20),
    )(*ins)


def owner_of(core, first, second):
    return jnp.where(core == 0, second * 4 + first, first * 4 + second)


def pair_sums(grads, received, m):
    rows, cols = received.shape[1:]

    def body(grads_ref, received_ref, *outs):
        zh, y, x, c = (lax.axis_index(name) for name in OWNERS)
        first, second = jnp.where(c == 0, x, y), jnp.where(c == 0, y, x)
        for half in range(2):

            def step(n, carry, half=half):
                i, j, z = n >> 3, (n >> 1) & 3, n & 1
                chip = owner_of(
                    c, first ^ place(2 * half + i, NEAR[m]), second ^ place(j, SECOND_NEAR[m])
                )
                chip = chip + (zh ^ z) * 16
                total = grads_ref[m, chip, c].astype(F32) + received_ref[chip].astype(F32)
                outs[half][i, j, z] = total.astype(BF16)
                return carry

            lax.fori_loop(0, 16, step, 0)

    return local(body, [grads, received], [((2, 4, 2, rows, cols), BF16)] * 2, 20)


def all_rows(own, other, m, pieces):
    rows, cols = own[0][0].shape[3:]
    part = 2 * rows // pieces

    def body(*refs):
        zh, y, x, c = (lax.axis_index(name) for name in OWNERS)
        out_ref = refs[7]
        for source in range(2):
            core = c if source == 0 else 1 - c
            first, second = jnp.where(core == 0, x, y), jnp.where(core == 0, y, x)
            for h in range(2):
                for p in range(2):

                    def step(n, carry, source=source, h=h, p=p, core=core, first=first, second=second):
                        i, j, z = n >> 2, (n >> 1) & 1, n & 1
                        if h == 0:
                            mask_a = 3 * i if p == 0 else 1 + i
                            mask_b = j
                        else:
                            mask_a = i if p == 0 else 3 - i
                            mask_b = 3 - j
                        chip = owner_of(core, first ^ mask_a, second ^ mask_b)
                        if source == 0:
                            value = refs[2 * h + p][i, j, z]
                        elif p == 0:
                            value = refs[4][h, i, j, z]
                        else:
                            value = refs[5 + h][i, j, z]
                        if m == 0:
                            out_ref[(zh ^ z) * 32 + chip * 2 + core] = value
                        else:
                            for q in range(rows // part):
                                at = z * (rows // part) + q
                                out_ref[at, chip * 2 + core] = value[q * part : (q + 1) * part]
                        return carry

                    lax.fori_loop(0, 8, step, 0)

    shape = (64, rows, cols) if m == 0 else (pieces, 32, part, cols)
    return local(body, [*own[0], *own[1], *other], [(shape, BF16)], 16)[0]


def dot(a, b, a_dim=1, b_dim=0):
    return lax.dot_general(a, b, (((a_dim,), (b_dim,)), ((), ())), preferred_element_type=F32)


def prepare(acts_parts, queries, keys, docs_row, docs_col, rows):
    count, width = acts_parts[0].shape
    heads = queries.shape[1] // HD
    part = rows // 2
    group = 16 * rows

    def body(*refs):
        query_ref, key_ref, row_ref, col_ref = refs[4:8]
        normed_ref, turned_ref, gram_ref, probs_ref, moved_ref, full_ref = refs[8:]
        here, zh = lax.axis_index("mp"), lax.axis_index("zh")
        for k in range(4):
            full_ref[:, pl.ds(pl.multiple_of((here ^ k) * width, 128), width)] = refs[k][...]
        rows_f = full_ref[...].astype(F32)
        mean = jnp.mean(rows_f * rows_f, axis=-1, keepdims=True)
        normed = (rows_f * lax.rsqrt(mean + norm_eps)).astype(BF16)
        normed_ref[...] = normed
        turned_ref[...] = jnp.transpose(normed.astype(F32)).astype(BF16)
        gram_ref[...] = dot(normed, normed, 1, 1)
        row_pos = lax.broadcasted_iota(jnp.int32, (count, count), 0)
        col_pos = lax.broadcasted_iota(jnp.int32, (count, count), 1)
        allowed = (row_pos >= col_pos) & (row_ref[...] == col_ref[...])
        for h in range(heads):
            span = slice(h * HD, (h + 1) * HD)
            scores = dot(query_ref[:, span], key_ref[:, span], 1, 1) * HD ** (-0.5)
            scores = jnp.where(allowed, scores, -1e30)
            raised = jnp.exp(scores - jnp.max(scores, axis=-1, keepdims=True))
            probs_ref[h] = (raised / jnp.sum(raised, axis=-1, keepdims=True)).astype(BF16)
        from_row = lax.broadcasted_iota(jnp.int32, (group, group // 2), 0)
        to_col = lax.broadcasted_iota(jnp.int32, (1, group // 2), 1)
        run = ((to_col.astype(F32) + 0.5) * (1.0 / part)).astype(jnp.int32)
        pick = (from_row == to_col + (run + (here & 1)) * part).astype(F32).astype(BF16)
        for g in range(2):
            start = (zh ^ (here >> 1)) * (2 * width) + g * group
            taken = dot(full_ref[:, pl.ds(pl.multiple_of(start, 128), group)], pick)
            moved = taken - pltpu.roll(taken, count - 1, 0)
            moved_ref[:, g * (group // 2) : (g + 1) * (group // 2)] = moved

    outs = [
        ((count, 4 * width), BF16),
        ((4 * width, count), BF16),
        ((count, count), F32),
        ((heads, count, count), BF16),
        ((count, width), F32),
    ]
    return local(
        body,
        [*acts_parts, queries, keys, docs_row, docs_col],
        outs,
        16,
        [pltpu.VMEM((count, 4 * width), BF16)],
    )


def quarters_of(both):
    rows, cols = both.shape[1:]
    part = rows // 2

    def body(both_ref, *outs):
        here = lax.axis_index("mp")
        for k in range(4):
            value = both_ref[(here ^ k) >> 1]
            odd = ((here ^ k) & 1) == 1
            outs[k][...] = jnp.where(odd, value[part:], value[:part])

    return local(body, [both], [((part, cols), BF16)] * 4, 4)


def attend(normed, value_proj, probs):
    count, width = normed.shape
    cols = value_proj.shape[1]

    def body(normed_ref, proj_ref, probs_ref, ctx_ref):
        values = (dot(normed_ref[...], proj_ref[...]) * width ** (-0.5)).astype(BF16)
        for h in range(cols // HD):
            span = slice(h * HD, (h + 1) * HD)
            ctx_ref[:, span] = dot(probs_ref[h], values[:, span]).astype(BF16)

    return local(body, [normed, value_proj, probs], [((count, cols), BF16)], 16)[0]


def first_branch(parts, out_proj):
    shape = (parts[0].shape[0], out_proj.shape[1])

    def body(*refs):
        total = dot(refs[0][...], refs[-2][0], 1, 1)
        for k in range(1, len(parts)):
            total = total + dot(refs[k][...], refs[-2][k], 1, 1)
        refs[-1][...] = total

    return local(body, [*parts, out_proj], [(shape, F32)], 16)[0]


def output_grad(branch, last, out_proj, moved):
    count, cols = last.shape
    scale = (4 * cols) ** (-0.5)

    def body(branch_ref, last_ref, proj_ref, moved_ref, *outs):
        total = (branch_ref[...] + dot(last_ref[...], proj_ref[3], 1, 1)) * scale
        dout = (moved_ref[...] + total).astype(BF16)
        for k in range(4):
            outs[k][...] = (dot(dout, proj_ref[k]) * scale).astype(outs[k].dtype)

    return local(
        body,
        [branch, last, out_proj, moved],
        [((count, cols), F32 if k == 0 else BF16) for k in range(4)],
        16,
    )


def values_grad(parts, probs, gram, width):
    count, cols = parts[0].shape

    def body(*refs):
        probs_ref, gram_ref, pulled_ref, squares_ref = refs[4:]
        total = refs[0][...]
        for k in range(1, 4):
            total = total + refs[k][...].astype(F32)
        dctx = total.astype(BF16)
        pulled = jnp.concatenate(
            [
                dot(probs_ref[h], dctx[:, h * HD : (h + 1) * HD], 0, 0).astype(BF16)
                for h in range(cols // HD)
            ],
            axis=1,
        )
        pulled_ref[...] = pulled
        product = gram_ref[...] * dot(pulled, pulled, 1, 1)
        total = jnp.sum(jnp.sum(product, axis=1, keepdims=True), axis=0, keepdims=True)
        squares_ref[...] = jnp.broadcast_to(total / width, (8, 128))

    return local(
        body, [*parts, probs, gram], [((count, cols), BF16), ((8, 128), F32)], 8
    )


def weight_grad(turned, pulled):
    def body(turned_ref, pulled_ref, out_ref):
        out_ref[...] = dot(turned_ref[...], pulled_ref[...])

    return local(body, [turned, pulled], [((turned.shape[0], pulled.shape[1]), F32)], 16)[0]


def inner_update(grad, value_proj, squares, entries):
    width, cols = value_proj.shape
    steps = 12
    block = width // steps

    def body(grad_ref, proj_ref, squares_ref, out_ref, held, sems):
        rms = jnp.sqrt(squares_ref[0:1, 0:1] / entries + norm_eps)
        scale = inner_rate * width ** (-0.5) / rms
        copies = []
        for i in range(steps):
            span = pl.ds(i * block, block)
            held[span, :] = (proj_ref[span, :].astype(F32) - grad_ref[span, :] * scale).astype(BF16)
            copies.append(pltpu.make_async_copy(held.at[span, :], out_ref.at[span, :], sems.at[i]))
            copies[-1].start()
        for copy in copies:
            copy.wait()

    vmem = pl.BlockSpec(memory_space=pltpu.VMEM)
    return pl.pallas_call(
        body,
        in_specs=[vmem] * 3,
        out_specs=pl.BlockSpec(memory_space=pl.ANY),
        out_shape=jax.ShapeDtypeStruct((width, cols), BF16),
        scratch_shapes=[pltpu.VMEM((width, cols), BF16), pltpu.SemaphoreType.DMA((steps,))],
        compiler_params=pltpu.CompilerParams(vmem_limit_bytes=20 * 2**20),
    )(grad, value_proj, squares)


def shards(pseudo_grad, outer_params, momentum, acts, queries, keys, doc_ids):
    workers = lax.axis_size(OWNERS)
    groups = lax.axis_size("mp")
    c = lax.axis_index("c")
    matrices, rows, cols = outer_params.shape
    grads = pseudo_grad.reshape(matrices, 32, 2, rows, cols)

    received = []
    for m in range(matrices):
        send = lax.dynamic_slice(grads, (m, 0, 1 - c, 0, 0), (1, 32, 1, rows, cols))
        received.append(swap(send.reshape(32, rows, cols), "c"))
    kept = []
    for m in range(matrices):
        keep, send = pair_sums(grads, received[m], m)
        if m == 1:
            acts, old_outer, old_momentum, send = lax.optimization_barrier(
                (acts, outer_params, momentum, send)
            )
        got = plane_swap(send, NEAR[m], True)
        total = keep.astype(F32) + got.astype(F32)
        got = plane_swap(total[1].astype(BF16), NEAR[m] ^ 2, True)
        kept.append(total[0] + got.astype(F32))
    acts_parts = [acts] + [mp_swap(acts, k) for k in (1, 2, 3)]
    far_state = swap(old_outer - outer_rate * outer_beta**2 * old_momentum, "zh")
    normed, turned, gram, probs, moved = prepare(
        acts_parts, queries, keys, doc_ids.reshape(1, -1), doc_ids.reshape(-1, 1), rows
    )

    totals = []
    for m in range(matrices):
        near = SECOND_NEAR[m]
        got = plane_swap(kept[m][2:].astype(BF16), near, False)
        total = kept[m][:2] + got.astype(F32)
        got = plane_swap(total[1].astype(BF16), near ^ 2, False)
        totals.append(total[0] + got.astype(F32))
    total = jnp.stack(totals)
    got = swap(total.astype(BF16), "zh")
    delta = (total + got.astype(F32)[:, ::-1]) / workers
    new_momentum = outer_beta * momentum + delta[:, 0]
    new_outer = outer_params - outer_rate * (delta[:, 0] + outer_beta * new_momentum)
    other_outer = far_state - outer_rate * (1 + outer_beta) * delta[:, 1]
    weights = [
        jnp.stack([new_outer[m].astype(BF16), other_outer[m].astype(BF16)]) for m in range(matrices)
    ]
    gathered = []
    for m in range(matrices):
        both = weights[m]
        if m == 1:
            taken = quarters_of(both)
            taken = [taken[0]] + [mp_swap(taken[k], k) for k in range(1, groups)]
            both = jnp.stack(taken).reshape(both.shape)
        two = jnp.stack([both, plane_swap(both, 1, False)])
        rest = plane_swap(two, 3, False)
        fore = jnp.stack([two, plane_swap(two, 3, True)])
        hind = jnp.stack([rest, plane_swap(rest, 1, True)])
        fore_rest = plane_swap(fore, 1, True)
        hind_rest = plane_swap(hind, 3, True)
        other = [swap(jnp.stack([fore, hind]), "c")]
        other.append(swap(fore_rest, "c"))
        other.append(swap(hind_rest, "c"))
        own = [[fore, fore_rest], [hind, hind_rest]]
        gathered.append(all_rows(own, other, m, groups))
    width = 64 * rows
    value_proj = gathered[0].reshape(width, cols)
    out_proj = gathered[1].reshape(groups, width // groups, cols)

    ctx = attend(normed, value_proj, probs)
    ctx_parts = []
    for k in (1, 2, 3):
        ctx_parts.append(mp_swap(ctx, k))
    branch = first_branch([ctx, *ctx_parts[:2]], out_proj)
    mine, *sends = output_grad(branch, ctx_parts[2], out_proj, moved)
    dctx_parts = [mine] + [mp_swap(sends[k - 1], k) for k in (3, 2, 1)]
    pulled, squares = values_grad(dctx_parts, probs, gram, width)
    grad = weight_grad(turned, pulled)
    squares = squares + mp_swap(squares, 2)
    squares = squares + mp_swap(squares, 1)
    new_local = inner_update(grad, value_proj, squares, width * cols * groups)
    return (new_outer, new_momentum, new_local[None])


def solution(mesh):
    fine = Mesh(mesh.devices.reshape(2, 4, 4, 2, 4), (*OWNERS, "mp"))
    placed = (
        P(OWNERS, None, None, "mp"),
        P(None, OWNERS, "mp"),
        P(None, OWNERS, "mp"),
        P(OWNERS, "mp"),
        P(OWNERS, "mp"),
        P(OWNERS, "mp"),
        P(OWNERS),
    )

    return jax.shard_map(
        shards,
        mesh=fine,
        in_specs=placed,
        out_specs=(P(None, OWNERS, "mp"), P(None, OWNERS, "mp"), P(OWNERS, None, "mp")),
        check_vma=False,
    )
```

```python
import jax
import jax.numpy as jnp
from jax import lax
from jax.experimental import pallas as pl
from jax.experimental.pallas import tpu as pltpu
from jax.sharding import Mesh, PartitionSpec as P


HD = 256

norm_eps = 1e-06
outer_rate = 0.7
outer_beta = 0.9
inner_rate = 0.1


PLANE = ("y", "x", "c")
OWNERS = ("zh", "y", "x", "c")
F32 = jnp.float32
BF16 = jnp.bfloat16
NEAR = (1, 3)
SECOND_NEAR = (3, 1)


def place(n, near):
    gray = n ^ (n >> 1)
    return gray if near == 3 else (3 * gray) & 3


def plane_swap(value, mask, first):
    pairs = []
    for y in range(4):
        for x in range(4):
            for c in range(2):
                along_x = (c == 0) == first
                ny, nx = (y, x ^ mask) if along_x else (y ^ mask, x)
                pairs.append(((y * 4 + x) * 2 + c, (ny * 4 + nx) * 2 + c))
    return lax.ppermute(value, PLANE, pairs)


def swap(value, axis):
    return lax.ppermute(value, axis, [(0, 1), (1, 0)])


def mp_swap(value, mask):
    return lax.ppermute(value, "mp", [(i, i ^ mask) for i in range(4)])


def local(body, ins, outs, mib, scratch=()):
    spec = pl.BlockSpec(memory_space=pltpu.VMEM)
    return pl.pallas_call(
        body,
        in_specs=[spec] * len(ins),
        out_specs=[spec] * len(outs),
        out_shape=[jax.ShapeDtypeStruct(shape, dtype) for shape, dtype in outs],
        scratch_shapes=scratch,
        compiler_params=pltpu.CompilerParams(vmem_limit_bytes=mib * 2**20),
    )(*ins)


def owner_of(core, first, second):
    return jnp.where(core == 0, second * 4 + first, first * 4 + second)


def pair_sums(grads, received, m):
    rows, cols = received.shape[1:]

    def body(grads_ref, received_ref, *outs):
        zh, y, x, c = (lax.axis_index(name) for name in OWNERS)
        first, second = jnp.where(c == 0, x, y), jnp.where(c == 0, y, x)
        for n0 in range(4):

            def step(n, carry, n0=n0):
                j, z = n >> 1, n & 1
                chip = owner_of(
                    c, first ^ place(n0, NEAR[m]), second ^ place(j, SECOND_NEAR[m])
                )
                chip = chip + (zh ^ z) * 16
                total = grads_ref[m, chip, c].astype(F32) + received_ref[chip].astype(F32)
                outs[n0][j, z] = total.astype(BF16)
                return carry

            lax.fori_loop(0, 8, step, 0)

    return local(body, [grads, received], [((4, 2, rows, cols), BF16)] * 4, 20)


def all_rows(own, other, m, pieces):
    rows, cols = own[0][0].shape[3:]
    part = 2 * rows // pieces

    def body(*refs):
        zh, y, x, c = (lax.axis_index(name) for name in OWNERS)
        out_ref = refs[7]
        for source in range(2):
            core = c if source == 0 else 1 - c
            first, second = jnp.where(core == 0, x, y), jnp.where(core == 0, y, x)
            for h in range(2):
                for p in range(2):

                    def step(n, carry, source=source, h=h, p=p, core=core, first=first, second=second):
                        i, j, z = n >> 2, (n >> 1) & 1, n & 1
                        if h == 0:
                            mask_a = 3 * i if p == 0 else 1 + i
                            mask_b = j
                        else:
                            mask_a = i if p == 0 else 3 - i
                            mask_b = 3 - j
                        chip = owner_of(core, first ^ mask_a, second ^ mask_b)
                        if source == 0:
                            value = refs[2 * h + p][i, j, z]
                        elif p == 0:
                            value = refs[4][h, i, j, z]
                        else:
                            value = refs[5 + h][i, j, z]
                        if m == 0:
                            out_ref[(zh ^ z) * 32 + chip * 2 + core] = value
                        else:
                            for q in range(rows // part):
                                at = z * (rows // part) + q
                                out_ref[at, chip * 2 + core] = value[q * part : (q + 1) * part]
                        return carry

                    lax.fori_loop(0, 8, step, 0)

    shape = (64, rows, cols) if m == 0 else (pieces, 32, part, cols)
    return local(body, [*own[0], *own[1], *other], [(shape, BF16)], 16)[0]


def dot(a, b, a_dim=1, b_dim=0):
    return lax.dot_general(a, b, (((a_dim,), (b_dim,)), ((), ())), preferred_element_type=F32)


def prepare(acts_parts, queries, keys, docs_row, docs_col, rows):
    count, width = acts_parts[0].shape
    heads = queries.shape[1] // HD
    part = rows // 2
    group = 16 * rows

    def body(*refs):
        query_ref, key_ref, row_ref, col_ref = refs[4:8]
        normed_ref, turned_ref, gram_ref, probs_ref, moved_ref, full_ref = refs[8:]
        here, zh = lax.axis_index("mp"), lax.axis_index("zh")
        for k in range(4):
            full_ref[:, pl.ds(pl.multiple_of((here ^ k) * width, 128), width)] = refs[k][...]
        rows_f = full_ref[...].astype(F32)
        mean = jnp.mean(rows_f * rows_f, axis=-1, keepdims=True)
        normed = (rows_f * lax.rsqrt(mean + norm_eps)).astype(BF16)
        normed_ref[...] = normed
        turned_ref[...] = jnp.transpose(normed.astype(F32)).astype(BF16)
        gram_ref[...] = dot(normed, normed, 1, 1)
        row_pos = lax.broadcasted_iota(jnp.int32, (count, count), 0)
        col_pos = lax.broadcasted_iota(jnp.int32, (count, count), 1)
        allowed = (row_pos >= col_pos) & (row_ref[...] == col_ref[...])
        for h in range(heads):
            span = slice(h * HD, (h + 1) * HD)
            scores = dot(query_ref[:, span], key_ref[:, span], 1, 1) * HD ** (-0.5)
            scores = jnp.where(allowed, scores, -1e30)
            raised = jnp.exp(scores - jnp.max(scores, axis=-1, keepdims=True))
            probs_ref[h] = (raised / jnp.sum(raised, axis=-1, keepdims=True)).astype(BF16)
        from_row = lax.broadcasted_iota(jnp.int32, (group, group // 2), 0)
        to_col = lax.broadcasted_iota(jnp.int32, (1, group // 2), 1)
        run = ((to_col.astype(F32) + 0.5) * (1.0 / part)).astype(jnp.int32)
        pick = (from_row == to_col + (run + (here & 1)) * part).astype(F32).astype(BF16)
        for g in range(2):
            start = (zh ^ (here >> 1)) * (2 * width) + g * group
            taken = dot(full_ref[:, pl.ds(pl.multiple_of(start, 128), group)], pick)
            moved = taken - pltpu.roll(taken, count - 1, 0)
            moved_ref[:, g * (group // 2) : (g + 1) * (group // 2)] = moved

    outs = [
        ((count, 4 * width), BF16),
        ((4 * width, count), BF16),
        ((count, count), F32),
        ((heads, count, count), BF16),
        ((count, width), F32),
    ]
    return local(
        body,
        [*acts_parts, queries, keys, docs_row, docs_col],
        outs,
        16,
        [pltpu.VMEM((count, 4 * width), BF16)],
    )


def quarters_of(both):
    rows, cols = both.shape[1:]
    part = rows // 2

    def body(both_ref, *outs):
        here = lax.axis_index("mp")
        for k in range(4):
            value = both_ref[(here ^ k) >> 1]
            odd = ((here ^ k) & 1) == 1
            outs[k][...] = jnp.where(odd, value[part:], value[:part])

    return local(body, [both], [((part, cols), BF16)] * 4, 4)


def attend(normed, value_proj, probs):
    count, width = normed.shape
    cols = value_proj.shape[1]

    def body(normed_ref, proj_ref, probs_ref, ctx_ref):
        values = (dot(normed_ref[...], proj_ref[...]) * width ** (-0.5)).astype(BF16)
        for h in range(cols // HD):
            span = slice(h * HD, (h + 1) * HD)
            ctx_ref[:, span] = dot(probs_ref[h], values[:, span]).astype(BF16)

    return local(body, [normed, value_proj, probs], [((count, cols), BF16)], 16)[0]


def first_branch(parts, out_proj):
    shape = (parts[0].shape[0], out_proj.shape[1])

    def body(*refs):
        total = dot(refs[0][...], refs[-2][0], 1, 1)
        for k in range(1, len(parts)):
            total = total + dot(refs[k][...], refs[-2][k], 1, 1)
        refs[-1][...] = total

    return local(body, [*parts, out_proj], [(shape, F32)], 16)[0]


def output_grad(branch, last, out_proj, moved):
    count, cols = last.shape
    scale = (4 * cols) ** (-0.5)

    def body(branch_ref, last_ref, proj_ref, moved_ref, *outs):
        total = (branch_ref[...] + dot(last_ref[...], proj_ref[3], 1, 1)) * scale
        dout = (moved_ref[...] + total).astype(BF16)
        for k in range(4):
            outs[k][...] = (dot(dout, proj_ref[k]) * scale).astype(outs[k].dtype)

    return local(
        body,
        [branch, last, out_proj, moved],
        [((count, cols), F32 if k == 0 else BF16) for k in range(4)],
        16,
    )


def values_grad(parts, probs, gram, width):
    count, cols = parts[0].shape

    def body(*refs):
        probs_ref, gram_ref, pulled_ref, squares_ref = refs[4:]
        total = refs[0][...]
        for k in range(1, 4):
            total = total + refs[k][...].astype(F32)
        dctx = total.astype(BF16)
        pulled = jnp.concatenate(
            [
                dot(probs_ref[h], dctx[:, h * HD : (h + 1) * HD], 0, 0).astype(BF16)
                for h in range(cols // HD)
            ],
            axis=1,
        )
        pulled_ref[...] = pulled
        product = gram_ref[...] * dot(pulled, pulled, 1, 1)
        total = jnp.sum(jnp.sum(product, axis=1, keepdims=True), axis=0, keepdims=True)
        squares_ref[...] = jnp.broadcast_to(total / width, (8, 128))

    return local(
        body, [*parts, probs, gram], [((count, cols), BF16), ((8, 128), F32)], 8
    )


def weight_grad(turned, pulled):
    def body(turned_ref, pulled_ref, out_ref):
        out_ref[...] = dot(turned_ref[...], pulled_ref[...])

    return local(body, [turned, pulled], [((turned.shape[0], pulled.shape[1]), F32)], 16)[0]


def inner_update(grad, value_proj, squares, entries):
    width, cols = value_proj.shape
    steps = 12
    block = width // steps

    def body(grad_ref, proj_ref, squares_ref, out_ref, held, sems):
        rms = jnp.sqrt(squares_ref[0:1, 0:1] / entries + norm_eps)
        scale = inner_rate * width ** (-0.5) / rms
        copies = []
        for i in range(steps):
            span = pl.ds(i * block, block)
            held[span, :] = (proj_ref[span, :].astype(F32) - grad_ref[span, :] * scale).astype(BF16)
            copies.append(pltpu.make_async_copy(held.at[span, :], out_ref.at[span, :], sems.at[i]))
            copies[-1].start()
        for copy in copies:
            copy.wait()

    vmem = pl.BlockSpec(memory_space=pltpu.VMEM)
    return pl.pallas_call(
        body,
        in_specs=[vmem] * 3,
        out_specs=pl.BlockSpec(memory_space=pl.ANY),
        out_shape=jax.ShapeDtypeStruct((width, cols), BF16),
        scratch_shapes=[pltpu.VMEM((width, cols), BF16), pltpu.SemaphoreType.DMA((steps,))],
        compiler_params=pltpu.CompilerParams(vmem_limit_bytes=20 * 2**20),
    )(grad, value_proj, squares)


def shards(pseudo_grad, outer_params, momentum, acts, queries, keys, doc_ids):
    workers = lax.axis_size(OWNERS)
    groups = lax.axis_size("mp")
    c = lax.axis_index("c")
    matrices, rows, cols = outer_params.shape
    grads = pseudo_grad.reshape(matrices, 32, 2, rows, cols)

    received, source = [], grads
    for m in range(matrices):
        send = lax.dynamic_slice(source, (m, 0, 1 - c, 0, 0), (1, 32, 1, rows, cols)).reshape(
            32, rows, cols
        )
        if m == 0:
            source, send = lax.optimization_barrier((source, send))
        received.append(swap(send, "c"))
    kept = []
    for m in range(matrices):
        near = NEAR[m]
        sums = pair_sums(grads, received[m], m)
        if m == 1:
            acts, old_outer, old_momentum, sums = lax.optimization_barrier(
                (acts, outer_params, momentum, sums)
            )
        got = plane_swap(sums[3], near, True)
        far = sums[1].astype(F32) + got.astype(F32)
        got = plane_swap(sums[2], near, True)
        total = sums[0].astype(F32) + got.astype(F32)
        got = plane_swap(far.astype(BF16), near ^ 2, True)
        kept.append(total + got.astype(F32))
    acts_parts = [acts] + [mp_swap(acts, k) for k in (1, 2, 3)]
    far_state = swap(old_outer - outer_rate * outer_beta**2 * old_momentum, "zh")
    normed, turned, gram, probs, moved = prepare(
        acts_parts, queries, keys, doc_ids.reshape(1, -1), doc_ids.reshape(-1, 1), rows
    )

    totals = []
    for m in range(matrices):
        near = SECOND_NEAR[m]
        got = plane_swap(kept[m][2:].astype(BF16), near, False)
        total = kept[m][:2] + got.astype(F32)
        got = plane_swap(total[1].astype(BF16), near ^ 2, False)
        totals.append(total[0] + got.astype(F32))
    total = jnp.stack(totals)
    got = swap(total.astype(BF16), "zh")
    delta = (total + got.astype(F32)[:, ::-1]) / workers
    new_momentum = outer_beta * momentum + delta[:, 0]
    new_outer = outer_params - outer_rate * (delta[:, 0] + outer_beta * new_momentum)
    other_outer = far_state - outer_rate * (1 + outer_beta) * delta[:, 1]
    weights = [
        jnp.stack([new_outer[m].astype(BF16), other_outer[m].astype(BF16)]) for m in range(matrices)
    ]
    gathered = []
    for m in range(matrices):
        both = weights[m]
        if m == 1:
            taken = quarters_of(both)
            taken = [taken[0]] + [mp_swap(taken[k], k) for k in range(1, groups)]
            both = jnp.stack(taken).reshape(both.shape)
        two = jnp.stack([both, plane_swap(both, 1, False)])
        rest = plane_swap(two, 3, False)
        fore = jnp.stack([two, plane_swap(two, 3, True)])
        hind = jnp.stack([rest, plane_swap(rest, 1, True)])
        fore_rest = plane_swap(fore, 1, True)
        hind_rest = plane_swap(hind, 3, True)
        other = [swap(jnp.stack([fore, hind]), "c")]
        other.append(swap(fore_rest, "c"))
        other.append(swap(hind_rest, "c"))
        own = [[fore, fore_rest], [hind, hind_rest]]
        gathered.append(all_rows(own, other, m, groups))
    width = 64 * rows
    value_proj = gathered[0].reshape(width, cols)
    out_proj = gathered[1].reshape(groups, width // groups, cols)

    ctx = attend(normed, value_proj, probs)
    ctx_parts = []
    for k in (1, 2, 3):
        ctx_parts.append(mp_swap(ctx, k))
    branch = first_branch([ctx, *ctx_parts[:2]], out_proj)
    mine, *sends = output_grad(branch, ctx_parts[2], out_proj, moved)
    dctx_parts = [mine] + [mp_swap(sends[k - 1], k) for k in (3, 2, 1)]
    pulled, squares = values_grad(dctx_parts, probs, gram, width)
    grad = weight_grad(turned, pulled)
    squares = squares + mp_swap(squares, 2)
    squares = squares + mp_swap(squares, 1)
    new_local = inner_update(grad, value_proj, squares, width * cols * groups)
    return (new_outer, new_momentum, new_local[None])


def solution(mesh):
    fine = Mesh(mesh.devices.reshape(2, 4, 4, 2, 4), (*OWNERS, "mp"))
    placed = (
        P(OWNERS, None, None, "mp"),
        P(None, OWNERS, "mp"),
        P(None, OWNERS, "mp"),
        P(OWNERS, "mp"),
        P(OWNERS, "mp"),
        P(OWNERS, "mp"),
        P(OWNERS),
    )

    return jax.shard_map(
        shards,
        mesh=fine,
        in_specs=placed,
        out_specs=(P(None, OWNERS, "mp"), P(None, OWNERS, "mp"), P(OWNERS, None, "mp")),
        check_vma=False,
    )
```

```python
import jax
import jax.numpy as jnp
from jax import lax
from jax.experimental import pallas as pl
from jax.experimental.pallas import tpu as pltpu
from jax.sharding import Mesh, PartitionSpec as P


HD = 256

norm_eps = 1e-06
outer_rate = 0.7
outer_beta = 0.9
inner_rate = 0.1


PLANE = ("y", "x", "c")
OWNERS = ("zh", "y", "x", "c")
F32 = jnp.float32
BF16 = jnp.bfloat16
NEAR = (1, 3)
SECOND_NEAR = (3, 1)


def place(n, near):
    gray = n ^ (n >> 1)
    return gray if near == 3 else (3 * gray) & 3


def plane_swap(value, mask, first):
    pairs = []
    for y in range(4):
        for x in range(4):
            for c in range(2):
                along_x = (c == 0) == first
                ny, nx = (y, x ^ mask) if along_x else (y ^ mask, x)
                pairs.append(((y * 4 + x) * 2 + c, (ny * 4 + nx) * 2 + c))
    return lax.ppermute(value, PLANE, pairs)


def swap(value, axis):
    return lax.ppermute(value, axis, [(0, 1), (1, 0)])


def mp_swap(value, mask):
    return lax.ppermute(value, "mp", [(i, i ^ mask) for i in range(4)])


def local(body, ins, outs, mib, scratch=()):
    spec = pl.BlockSpec(memory_space=pltpu.VMEM)
    return pl.pallas_call(
        body,
        in_specs=[spec] * len(ins),
        out_specs=[spec] * len(outs),
        out_shape=[jax.ShapeDtypeStruct(shape, dtype) for shape, dtype in outs],
        scratch_shapes=scratch,
        compiler_params=pltpu.CompilerParams(vmem_limit_bytes=mib * 2**20),
    )(*ins)


def owner_of(core, first, second):
    return jnp.where(core == 0, second * 4 + first, first * 4 + second)


def pair_sums(grads, received, m):
    rows, cols = received.shape[1:]

    def body(grads_ref, received_ref, *outs):
        zh, y, x, c = (lax.axis_index(name) for name in OWNERS)
        first, second = jnp.where(c == 0, x, y), jnp.where(c == 0, y, x)
        for n0 in range(4):

            def step(n, carry, n0=n0):
                j, z = n >> 1, n & 1
                chip = owner_of(
                    c, first ^ place(n0, NEAR[m]), second ^ place(j, SECOND_NEAR[m])
                )
                chip = chip + (zh ^ z) * 16
                total = grads_ref[m, chip, c].astype(F32) + received_ref[chip].astype(F32)
                outs[n0][j, z] = total.astype(BF16)
                return carry

            lax.fori_loop(0, 8, step, 0)

    return local(body, [grads, received], [((4, 2, rows, cols), BF16)] * 4, 20)


def all_rows(own, other, m, pieces):
    rows, cols = own[0][0].shape[3:]
    part = 2 * rows // pieces

    def body(*refs):
        zh, y, x, c = (lax.axis_index(name) for name in OWNERS)
        out_ref = refs[7]
        for source in range(2):
            core = c if source == 0 else 1 - c
            first, second = jnp.where(core == 0, x, y), jnp.where(core == 0, y, x)
            for h in range(2):
                for p in range(2):

                    def step(n, carry, source=source, h=h, p=p, core=core, first=first, second=second):
                        i, j, z = n >> 2, (n >> 1) & 1, n & 1
                        if h == 0:
                            mask_a = 3 * i if p == 0 else 1 + i
                            mask_b = j
                        else:
                            mask_a = i if p == 0 else 3 - i
                            mask_b = 3 - j
                        chip = owner_of(core, first ^ mask_a, second ^ mask_b)
                        if source == 0:
                            value = refs[2 * h + p][i, j, z]
                        elif p == 0:
                            value = refs[4][h, i, j, z]
                        else:
                            value = refs[5 + h][i, j, z]
                        if m == 0:
                            out_ref[(zh ^ z) * 32 + chip * 2 + core] = value
                        else:
                            for q in range(rows // part):
                                at = z * (rows // part) + q
                                out_ref[at, chip * 2 + core] = value[q * part : (q + 1) * part]
                        return carry

                    lax.fori_loop(0, 8, step, 0)

    shape = (64, rows, cols) if m == 0 else (pieces, 32, part, cols)
    return local(body, [*own[0], *own[1], *other], [(shape, BF16)], 16)[0]


def dot(a, b, a_dim=1, b_dim=0):
    return lax.dot_general(a, b, (((a_dim,), (b_dim,)), ((), ())), preferred_element_type=F32)


def prepare(acts_parts, queries, keys, docs_row, docs_col, rows):
    count, width = acts_parts[0].shape
    heads = queries.shape[1] // HD
    part = rows // 2
    group = 16 * rows

    def body(*refs):
        query_ref, key_ref, row_ref, col_ref = refs[4:8]
        normed_ref, turned_ref, gram_ref, probs_ref, moved_ref, full_ref = refs[8:]
        here, zh = lax.axis_index("mp"), lax.axis_index("zh")
        for k in range(4):
            full_ref[:, pl.ds(pl.multiple_of((here ^ k) * width, 128), width)] = refs[k][...]
        rows_f = full_ref[...].astype(F32)
        mean = jnp.mean(rows_f * rows_f, axis=-1, keepdims=True)
        normed = (rows_f * lax.rsqrt(mean + norm_eps)).astype(BF16)
        normed_ref[...] = normed
        turned_ref[...] = jnp.transpose(normed.astype(F32)).astype(BF16)
        gram_ref[...] = dot(normed, normed, 1, 1)
        row_pos = lax.broadcasted_iota(jnp.int32, (count, count), 0)
        col_pos = lax.broadcasted_iota(jnp.int32, (count, count), 1)
        allowed = (row_pos >= col_pos) & (row_ref[...] == col_ref[...])
        for h in range(heads):
            span = slice(h * HD, (h + 1) * HD)
            scores = dot(query_ref[:, span], key_ref[:, span], 1, 1) * HD ** (-0.5)
            scores = jnp.where(allowed, scores, -1e30)
            raised = jnp.exp(scores - jnp.max(scores, axis=-1, keepdims=True))
            probs_ref[h] = (raised / jnp.sum(raised, axis=-1, keepdims=True)).astype(BF16)
        from_row = lax.broadcasted_iota(jnp.int32, (group, group // 2), 0)
        to_col = lax.broadcasted_iota(jnp.int32, (1, group // 2), 1)
        run = ((to_col.astype(F32) + 0.5) * (1.0 / part)).astype(jnp.int32)
        pick = (from_row == to_col + (run + (here & 1)) * part).astype(F32).astype(BF16)
        for g in range(2):
            start = (zh ^ (here >> 1)) * (2 * width) + g * group
            taken = dot(full_ref[:, pl.ds(pl.multiple_of(start, 128), group)], pick)
            moved = taken - pltpu.roll(taken, count - 1, 0)
            moved_ref[:, g * (group // 2) : (g + 1) * (group // 2)] = moved

    outs = [
        ((count, 4 * width), BF16),
        ((4 * width, count), BF16),
        ((count, count), F32),
        ((heads, count, count), BF16),
        ((count, width), F32),
    ]
    return local(
        body,
        [*acts_parts, queries, keys, docs_row, docs_col],
        outs,
        16,
        [pltpu.VMEM((count, 4 * width), BF16)],
    )


def quarters_of(both):
    rows, cols = both.shape[1:]
    part = rows // 2

    def body(both_ref, *outs):
        here = lax.axis_index("mp")
        for k in range(4):
            value = both_ref[(here ^ k) >> 1]
            odd = ((here ^ k) & 1) == 1
            outs[k][...] = jnp.where(odd, value[part:], value[:part])

    return local(body, [both], [((part, cols), BF16)] * 4, 4)


def attend(normed, value_proj, probs):
    count, width = normed.shape
    cols = value_proj.shape[1]

    def body(normed_ref, proj_ref, probs_ref, ctx_ref):
        values = (dot(normed_ref[...], proj_ref[...]) * width ** (-0.5)).astype(BF16)
        for h in range(cols // HD):
            span = slice(h * HD, (h + 1) * HD)
            ctx_ref[:, span] = dot(probs_ref[h], values[:, span]).astype(BF16)

    return local(body, [normed, value_proj, probs], [((count, cols), BF16)], 16)[0]


def first_branch(parts, out_proj):
    shape = (parts[0].shape[0], out_proj.shape[1])

    def body(*refs):
        total = dot(refs[0][...], refs[-2][0], 1, 1)
        for k in range(1, len(parts)):
            total = total + dot(refs[k][...], refs[-2][k], 1, 1)
        refs[-1][...] = total

    return local(body, [*parts, out_proj], [(shape, F32)], 16)[0]


def output_grad(branch, last, out_proj, moved):
    count, cols = last.shape
    scale = (4 * cols) ** (-0.5)

    def body(branch_ref, last_ref, proj_ref, moved_ref, *outs):
        total = (branch_ref[...] + dot(last_ref[...], proj_ref[3], 1, 1)) * scale
        dout = (moved_ref[...] + total).astype(BF16)
        for k in range(4):
            outs[k][...] = (dot(dout, proj_ref[k]) * scale).astype(outs[k].dtype)

    return local(
        body,
        [branch, last, out_proj, moved],
        [((count, cols), F32 if k == 0 else BF16) for k in range(4)],
        16,
    )


def values_grad(parts, probs, gram, width):
    count, cols = parts[0].shape

    def body(*refs):
        probs_ref, gram_ref, pulled_ref, squares_ref = refs[4:]
        total = refs[0][...]
        for k in range(1, 4):
            total = total + refs[k][...].astype(F32)
        dctx = total.astype(BF16)
        pulled = jnp.concatenate(
            [
                dot(probs_ref[h], dctx[:, h * HD : (h + 1) * HD], 0, 0).astype(BF16)
                for h in range(cols // HD)
            ],
            axis=1,
        )
        pulled_ref[...] = pulled
        product = gram_ref[...] * dot(pulled, pulled, 1, 1)
        total = jnp.sum(jnp.sum(product, axis=1, keepdims=True), axis=0, keepdims=True)
        squares_ref[...] = jnp.broadcast_to(total / width, (8, 128))

    return local(
        body, [*parts, probs, gram], [((count, cols), BF16), ((8, 128), F32)], 8
    )


def weight_grad(turned, pulled):
    def body(turned_ref, pulled_ref, out_ref):
        out_ref[...] = dot(turned_ref[...], pulled_ref[...])

    return local(body, [turned, pulled], [((turned.shape[0], pulled.shape[1]), F32)], 16)[0]


def inner_update(grad, value_proj, squares, entries):
    width, cols = value_proj.shape
    steps = 12
    block = width // steps

    def body(grad_ref, proj_ref, squares_ref, out_ref, held, sems):
        rms = jnp.sqrt(squares_ref[0:1, 0:1] / entries + norm_eps)
        scale = inner_rate * width ** (-0.5) / rms
        copies = []
        for i in range(steps):
            span = pl.ds(i * block, block)
            held[span, :] = (proj_ref[span, :].astype(F32) - grad_ref[span, :] * scale).astype(BF16)
            copies.append(pltpu.make_async_copy(held.at[span, :], out_ref.at[span, :], sems.at[i]))
            copies[-1].start()
        for copy in copies:
            copy.wait()

    vmem = pl.BlockSpec(memory_space=pltpu.VMEM)
    return pl.pallas_call(
        body,
        in_specs=[vmem] * 3,
        out_specs=pl.BlockSpec(memory_space=pl.ANY),
        out_shape=jax.ShapeDtypeStruct((width, cols), BF16),
        scratch_shapes=[pltpu.VMEM((width, cols), BF16), pltpu.SemaphoreType.DMA((steps,))],
        compiler_params=pltpu.CompilerParams(vmem_limit_bytes=20 * 2**20),
    )(grad, value_proj, squares)


def shards(pseudo_grad, outer_params, momentum, acts, queries, keys, doc_ids):
    workers = lax.axis_size(OWNERS)
    groups = lax.axis_size("mp")
    c = lax.axis_index("c")
    matrices, rows, cols = outer_params.shape
    grads = pseudo_grad.reshape(matrices, 32, 2, rows, cols)

    received, source = [], grads
    for m in range(matrices):
        send = lax.dynamic_slice(source, (m, 0, 1 - c, 0, 0), (1, 32, 1, rows, cols)).reshape(
            32, rows, cols
        )
        if m == 0:
            source, send = lax.optimization_barrier((source, send))
        received.append(swap(send, "c"))
    kept = []
    for m in range(matrices):
        near = NEAR[m]
        sums = pair_sums(grads, received[m], m)
        if m == 1:
            acts, old_outer, old_momentum, sums = lax.optimization_barrier(
                (acts, outer_params, momentum, sums)
            )
        got = plane_swap(sums[3], near, True)
        far = sums[1].astype(F32) + got.astype(F32)
        got = plane_swap(sums[2], near, True)
        total = sums[0].astype(F32) + got.astype(F32)
        got = plane_swap(far.astype(BF16), near ^ 2, True)
        kept.append(total + got.astype(F32))
    acts_parts = [acts] + [mp_swap(acts, k) for k in (1, 2, 3)]
    far_state = swap(old_outer - outer_rate * outer_beta**2 * old_momentum, "zh")
    normed, turned, gram, probs, moved = prepare(
        acts_parts, queries, keys, doc_ids.reshape(1, -1), doc_ids.reshape(-1, 1), rows
    )

    totals = []
    for m in range(matrices):
        near = SECOND_NEAR[m]
        got = plane_swap(kept[m][2:].astype(BF16), near, False)
        total = kept[m][:2] + got.astype(F32)
        got = plane_swap(total[1].astype(BF16), near ^ 2, False)
        totals.append(total[0] + got.astype(F32))
    total = jnp.stack(totals)
    got = swap(total.astype(BF16), "zh")
    delta = (total + got.astype(F32)[:, ::-1]) / workers

    def outer_update(summed):
        moment_next = outer_beta * momentum + summed
        return outer_params - outer_rate * (summed + outer_beta * moment_next), moment_next

    here_outer, _ = outer_update(delta[:, 0])
    other_outer = far_state - outer_rate * (1 + outer_beta) * delta[:, 1]
    weights = [
        jnp.stack([here_outer[m].astype(BF16), other_outer[m].astype(BF16)]) for m in range(matrices)
    ]
    gathered = []
    for m in range(matrices):
        both = weights[m]
        if m == 1:
            taken = quarters_of(both)
            got2 = mp_swap(jnp.stack([taken[2], taken[3]]), 2)
            got1 = mp_swap(jnp.stack([taken[1], got2[1]]), 1)
            both = jnp.stack([taken[0], got1[0], got2[0], got1[1]]).reshape(both.shape)
        two = jnp.stack([both, plane_swap(both, 1, False)])
        if m == 0:
            two, late = lax.optimization_barrier((two, delta[:, 0]))
            new_outer, new_momentum = outer_update(late)
        rest = plane_swap(two, 3, False)
        fore = jnp.stack([two, plane_swap(two, 3, True)])
        hind = jnp.stack([rest, plane_swap(rest, 1, True)])
        fore_rest = plane_swap(fore, 1, True)
        hind_rest = plane_swap(hind, 3, True)
        other = [swap(jnp.stack([fore, hind]), "c")]
        other.append(swap(fore_rest, "c"))
        other.append(swap(hind_rest, "c"))
        own = [[fore, fore_rest], [hind, hind_rest]]
        gathered.append(all_rows(own, other, m, groups))
    width = 64 * rows
    value_proj = gathered[0].reshape(width, cols)
    out_proj = gathered[1].reshape(groups, width // groups, cols)

    ctx = attend(normed, value_proj, probs)
    ctx_parts = []
    for k in (1, 2, 3):
        ctx_parts.append(mp_swap(ctx, k))
    branch = first_branch([ctx, *ctx_parts[:2]], out_proj)
    mine, *sends = output_grad(branch, ctx_parts[2], out_proj, moved)
    dctx_parts = [mine] + [mp_swap(sends[k - 1], k) for k in (3, 2, 1)]
    pulled, squares = values_grad(dctx_parts, probs, gram, width)
    grad = weight_grad(turned, pulled)
    squares = squares + mp_swap(squares, 2)
    squares = squares + mp_swap(squares, 1)
    new_local = inner_update(grad, value_proj, squares, width * cols * groups)
    return (new_outer, new_momentum, new_local[None])


def solution(mesh):
    fine = Mesh(mesh.devices.reshape(2, 4, 4, 2, 4), (*OWNERS, "mp"))
    placed = (
        P(OWNERS, None, None, "mp"),
        P(None, OWNERS, "mp"),
        P(None, OWNERS, "mp"),
        P(OWNERS, "mp"),
        P(OWNERS, "mp"),
        P(OWNERS, "mp"),
        P(OWNERS),
    )

    return jax.shard_map(
        shards,
        mesh=fine,
        in_specs=placed,
        out_specs=(P(None, OWNERS, "mp"), P(None, OWNERS, "mp"), P(OWNERS, None, "mp")),
        check_vma=False,
    )
```

```python
import jax
import jax.numpy as jnp
from jax import lax
from jax.experimental import pallas as pl
from jax.experimental.pallas import tpu as pltpu
from jax.sharding import Mesh, PartitionSpec as P


HD = 256

norm_eps = 1e-06
outer_rate = 0.7
outer_beta = 0.9
inner_rate = 0.1


PLANE = ("y", "x", "c")
OWNERS = ("zh", "y", "x", "c")
F32 = jnp.float32
BF16 = jnp.bfloat16
NEAR = (1, 3)
SECOND_NEAR = (3, 1)


def place(n, near):
    gray = n ^ (n >> 1)
    return gray if near == 3 else (3 * gray) & 3


def plane_swap(value, mask, first):
    pairs = []
    for y in range(4):
        for x in range(4):
            for c in range(2):
                along_x = (c == 0) == first
                ny, nx = (y, x ^ mask) if along_x else (y ^ mask, x)
                pairs.append(((y * 4 + x) * 2 + c, (ny * 4 + nx) * 2 + c))
    return lax.ppermute(value, PLANE, pairs)


def swap(value, axis):
    return lax.ppermute(value, axis, [(0, 1), (1, 0)])


def mp_swap(value, mask):
    return lax.ppermute(value, "mp", [(i, i ^ mask) for i in range(4)])


def local(body, ins, outs, mib, scratch=()):
    spec = pl.BlockSpec(memory_space=pltpu.VMEM)
    return pl.pallas_call(
        body,
        in_specs=[spec] * len(ins),
        out_specs=[spec] * len(outs),
        out_shape=[jax.ShapeDtypeStruct(shape, dtype) for shape, dtype in outs],
        scratch_shapes=scratch,
        compiler_params=pltpu.CompilerParams(vmem_limit_bytes=mib * 2**20),
    )(*ins)


def owner_of(core, first, second):
    return jnp.where(core == 0, second * 4 + first, first * 4 + second)


def pair_sums(grads, received, m):
    rows, cols = received.shape[1:]

    def body(grads_ref, received_ref, *outs):
        zh, y, x, c = (lax.axis_index(name) for name in OWNERS)
        first, second = jnp.where(c == 0, x, y), jnp.where(c == 0, y, x)
        for n0 in range(4):

            def step(n, carry, n0=n0):
                j, z = n >> 1, n & 1
                chip = owner_of(
                    c, first ^ place(n0, NEAR[m]), second ^ place(j, SECOND_NEAR[m])
                )
                chip = chip + (zh ^ z) * 16
                total = grads_ref[m, chip, c].astype(F32) + received_ref[chip].astype(F32)
                outs[n0][j, z] = total.astype(BF16)
                return carry

            lax.fori_loop(0, 8, step, 0)

    return local(body, [grads, received], [((4, 2, rows, cols), BF16)] * 4, 20)


def all_rows(own, other, m, pieces):
    rows, cols = own[0][0].shape[3:]
    part = 2 * rows // pieces

    def body(*refs):
        zh, y, x, c = (lax.axis_index(name) for name in OWNERS)
        out_ref = refs[7]
        for source in range(2):
            core = c if source == 0 else 1 - c
            first, second = jnp.where(core == 0, x, y), jnp.where(core == 0, y, x)
            for h in range(2):
                for p in range(2):

                    def step(n, carry, source=source, h=h, p=p, core=core, first=first, second=second):
                        i, j, z = n >> 2, (n >> 1) & 1, n & 1
                        if h == 0:
                            mask_a = 3 * i if p == 0 else 1 + i
                            mask_b = j
                        else:
                            mask_a = i if p == 0 else 3 - i
                            mask_b = 3 - j
                        chip = owner_of(core, first ^ mask_a, second ^ mask_b)
                        if source == 0:
                            value = refs[2 * h + p][i, j, z]
                        elif p == 0:
                            value = refs[4][h, i, j, z]
                        else:
                            value = refs[5 + h][i, j, z]
                        if m == 0:
                            out_ref[(zh ^ z) * 32 + chip * 2 + core] = value
                        else:
                            for q in range(rows // part):
                                at = z * (rows // part) + q
                                out_ref[at, chip * 2 + core] = value[q * part : (q + 1) * part]
                        return carry

                    lax.fori_loop(0, 8, step, 0)

    shape = (64, rows, cols) if m == 0 else (pieces, 32, part, cols)
    return local(body, [*own[0], *own[1], *other], [(shape, BF16)], 16)[0]


def dot(a, b, a_dim=1, b_dim=0):
    return lax.dot_general(a, b, (((a_dim,), (b_dim,)), ((), ())), preferred_element_type=F32)


def prepare(acts_parts, queries, keys, docs_row, docs_col, rows):
    count, width = acts_parts[0].shape
    heads = queries.shape[1] // HD
    part = rows // 2
    group = 16 * rows

    def body(*refs):
        query_ref, key_ref, row_ref, col_ref = refs[4:8]
        normed_ref, turned_ref, gram_ref, probs_ref, moved_ref, full_ref = refs[8:]
        here, zh = lax.axis_index("mp"), lax.axis_index("zh")
        for k in range(4):
            full_ref[:, pl.ds(pl.multiple_of((here ^ k) * width, 128), width)] = refs[k][...]
        rows_f = full_ref[...].astype(F32)
        mean = jnp.mean(rows_f * rows_f, axis=-1, keepdims=True)
        normed = (rows_f * lax.rsqrt(mean + norm_eps)).astype(BF16)
        normed_ref[...] = normed
        turned_ref[...] = jnp.transpose(normed.astype(F32)).astype(BF16)
        gram_ref[...] = dot(normed, normed, 1, 1)
        row_pos = lax.broadcasted_iota(jnp.int32, (count, count), 0)
        col_pos = lax.broadcasted_iota(jnp.int32, (count, count), 1)
        allowed = (row_pos >= col_pos) & (row_ref[...] == col_ref[...])
        for h in range(heads):
            span = slice(h * HD, (h + 1) * HD)
            scores = dot(query_ref[:, span], key_ref[:, span], 1, 1) * HD ** (-0.5)
            scores = jnp.where(allowed, scores, -1e30)
            raised = jnp.exp(scores - jnp.max(scores, axis=-1, keepdims=True))
            probs_ref[h] = (raised / jnp.sum(raised, axis=-1, keepdims=True)).astype(BF16)
        from_row = lax.broadcasted_iota(jnp.int32, (group, group // 2), 0)
        to_col = lax.broadcasted_iota(jnp.int32, (1, group // 2), 1)
        run = ((to_col.astype(F32) + 0.5) * (1.0 / part)).astype(jnp.int32)
        pick = (from_row == to_col + (run + (here & 1)) * part).astype(F32).astype(BF16)
        for g in range(2):
            start = (zh ^ (here >> 1)) * (2 * width) + g * group
            taken = dot(full_ref[:, pl.ds(pl.multiple_of(start, 128), group)], pick)
            moved = taken - pltpu.roll(taken, count - 1, 0)
            moved_ref[:, g * (group // 2) : (g + 1) * (group // 2)] = moved

    outs = [
        ((count, 4 * width), BF16),
        ((4 * width, count), BF16),
        ((count, count), F32),
        ((heads, count, count), BF16),
        ((count, width), F32),
    ]
    return local(
        body,
        [*acts_parts, queries, keys, docs_row, docs_col],
        outs,
        16,
        [pltpu.VMEM((count, 4 * width), BF16)],
    )


def quarters_of(both):
    rows, cols = both.shape[1:]
    part = rows // 2

    def body(both_ref, *outs):
        here = lax.axis_index("mp")
        for k in range(4):
            value = both_ref[(here ^ k) >> 1]
            odd = ((here ^ k) & 1) == 1
            outs[k][...] = jnp.where(odd, value[part:], value[:part])

    return local(body, [both], [((part, cols), BF16)] * 4, 4)


def attend(normed, value_proj, probs):
    count, width = normed.shape
    cols = value_proj.shape[1]

    def body(normed_ref, proj_ref, probs_ref, ctx_ref):
        values = (dot(normed_ref[...], proj_ref[...]) * width ** (-0.5)).astype(BF16)
        for h in range(cols // HD):
            span = slice(h * HD, (h + 1) * HD)
            ctx_ref[:, span] = dot(probs_ref[h], values[:, span]).astype(BF16)

    return local(body, [normed, value_proj, probs], [((count, cols), BF16)], 16)[0]


def first_branch(parts, out_proj):
    shape = (parts[0].shape[0], out_proj.shape[1])

    def body(*refs):
        total = dot(refs[0][...], refs[-2][0], 1, 1)
        for k in range(1, len(parts)):
            total = total + dot(refs[k][...], refs[-2][k], 1, 1)
        refs[-1][...] = total

    return local(body, [*parts, out_proj], [(shape, F32)], 16)[0]


def output_grad(branch, last, out_proj, moved):
    count, cols = last.shape
    scale = (4 * cols) ** (-0.5)

    def body(branch_ref, last_ref, proj_ref, moved_ref, *outs):
        total = (branch_ref[...] + dot(last_ref[...], proj_ref[3], 1, 1)) * scale
        dout = (moved_ref[...] + total).astype(BF16)
        for k in range(4):
            outs[k][...] = (dot(dout, proj_ref[k]) * scale).astype(outs[k].dtype)

    return local(
        body,
        [branch, last, out_proj, moved],
        [((count, cols), F32 if k == 0 else BF16) for k in range(4)],
        16,
    )


def values_grad(parts, probs, gram, width):
    count, cols = parts[0].shape

    def body(*refs):
        probs_ref, gram_ref, pulled_ref, squares_ref = refs[4:]
        total = refs[0][...]
        for k in range(1, 4):
            total = total + refs[k][...].astype(F32)
        dctx = total.astype(BF16)
        pulled = jnp.concatenate(
            [
                dot(probs_ref[h], dctx[:, h * HD : (h + 1) * HD], 0, 0).astype(BF16)
                for h in range(cols // HD)
            ],
            axis=1,
        )
        pulled_ref[...] = pulled
        product = gram_ref[...] * dot(pulled, pulled, 1, 1)
        total = jnp.sum(jnp.sum(product, axis=1, keepdims=True), axis=0, keepdims=True)
        squares_ref[...] = jnp.broadcast_to(total / width, (8, 128))

    return local(
        body, [*parts, probs, gram], [((count, cols), BF16), ((8, 128), F32)], 8
    )


def weight_grad(turned, pulled):
    def body(turned_ref, pulled_ref, out_ref):
        out_ref[...] = dot(turned_ref[...], pulled_ref[...])

    return local(body, [turned, pulled], [((turned.shape[0], pulled.shape[1]), F32)], 16)[0]


def inner_update(grad, value_proj, squares, entries):
    width, cols = value_proj.shape
    steps = 12
    block = width // steps

    def body(grad_ref, proj_ref, squares_ref, out_ref, held, sems):
        rms = jnp.sqrt(squares_ref[0:1, 0:1] / entries + norm_eps)
        scale = inner_rate * width ** (-0.5) / rms
        copies = []
        for i in range(steps):
            span = pl.ds(i * block, block)
            held[span, :] = (proj_ref[span, :].astype(F32) - grad_ref[span, :] * scale).astype(BF16)
            copies.append(pltpu.make_async_copy(held.at[span, :], out_ref.at[span, :], sems.at[i]))
            copies[-1].start()
        for copy in copies:
            copy.wait()

    vmem = pl.BlockSpec(memory_space=pltpu.VMEM)
    return pl.pallas_call(
        body,
        in_specs=[vmem] * 3,
        out_specs=pl.BlockSpec(memory_space=pl.ANY),
        out_shape=jax.ShapeDtypeStruct((width, cols), BF16),
        scratch_shapes=[pltpu.VMEM((width, cols), BF16), pltpu.SemaphoreType.DMA((steps,))],
        compiler_params=pltpu.CompilerParams(vmem_limit_bytes=20 * 2**20),
    )(grad, value_proj, squares)


def shards(pseudo_grad, outer_params, momentum, acts, queries, keys, doc_ids):
    workers = lax.axis_size(OWNERS)
    groups = lax.axis_size("mp")
    c = lax.axis_index("c")
    matrices, rows, cols = outer_params.shape
    grads = pseudo_grad.reshape(matrices, 32, 2, rows, cols)

    received, source = [], grads
    for m in range(matrices):
        send = lax.dynamic_slice(source, (m, 0, 1 - c, 0, 0), (1, 32, 1, rows, cols)).reshape(
            32, rows, cols
        )
        if m == 0:
            source, send = lax.optimization_barrier((source, send))
        received.append(swap(send, "c"))
    kept = []
    for m in range(matrices):
        near = NEAR[m]
        sums = pair_sums(grads, received[m], m)
        if m == 1:
            acts, old_outer, old_momentum, sums = lax.optimization_barrier(
                (acts, outer_params, momentum, sums)
            )
        got = plane_swap(sums[3], near, True)
        far = sums[1].astype(F32) + got.astype(F32)
        got = plane_swap(sums[2], near, True)
        total = sums[0].astype(F32) + got.astype(F32)
        got = plane_swap(far.astype(BF16), near ^ 2, True)
        kept.append(total + got.astype(F32))
    acts_parts = [acts] + [mp_swap(acts, k) for k in (1, 2, 3)]
    far_state = swap(old_outer - outer_rate * outer_beta**2 * old_momentum, "zh")
    normed, turned, gram, probs, moved = prepare(
        acts_parts, queries, keys, doc_ids.reshape(1, -1), doc_ids.reshape(-1, 1), rows
    )

    totals = []
    for m in range(matrices):
        near = SECOND_NEAR[m]
        got = plane_swap(kept[m][2:].astype(BF16), near, False)
        total = kept[m][:2] + got.astype(F32)
        got = plane_swap(total[1].astype(BF16), near ^ 2, False)
        totals.append(total[0] + got.astype(F32))
    total = jnp.stack(totals)
    got = swap(total.astype(BF16), "zh")
    delta = (total + got.astype(F32)[:, ::-1]) / workers

    def outer_update(summed):
        moment_next = outer_beta * momentum + summed
        return outer_params - outer_rate * (summed + outer_beta * moment_next), moment_next

    here_outer, _ = outer_update(delta[:, 0])
    other_outer = far_state - outer_rate * (1 + outer_beta) * delta[:, 1]
    weights = [
        jnp.stack([here_outer[m].astype(BF16), other_outer[m].astype(BF16)]) for m in range(matrices)
    ]
    gathered = []
    for m in range(matrices):
        both = weights[m]
        if m == 1:
            taken = quarters_of(both)
            got2 = mp_swap(jnp.stack([taken[2], taken[3]]), 2)
            far_one, far_two = got2[0], got2[1]
            got1 = mp_swap(jnp.stack([taken[1], far_two]), 1)
            both = jnp.stack([taken[0], got1[0], far_one, got1[1]]).reshape(both.shape)
        two = jnp.stack([both, plane_swap(both, 1, False)])
        if m == 0:
            two, late = lax.optimization_barrier((two, delta[:, 0]))
            new_outer, new_momentum = outer_update(late)
        rest = plane_swap(two, 3, False)
        fore = jnp.stack([two, plane_swap(two, 3, True)])
        hind = jnp.stack([rest, plane_swap(rest, 1, True)])
        fore_rest = plane_swap(fore, 1, True)
        hind_rest = plane_swap(hind, 3, True)
        other = [swap(jnp.stack([fore, hind]), "c")]
        other.append(swap(fore_rest, "c"))
        other.append(swap(hind_rest, "c"))
        own = [[fore, fore_rest], [hind, hind_rest]]
        gathered.append(all_rows(own, other, m, groups))
    width = 64 * rows
    value_proj = gathered[0].reshape(width, cols)
    out_proj = gathered[1].reshape(groups, width // groups, cols)

    ctx = attend(normed, value_proj, probs)
    ctx_parts = []
    for k in (1, 2, 3):
        ctx_parts.append(mp_swap(ctx, k))
    branch = first_branch([ctx, *ctx_parts[:2]], out_proj)
    mine, *sends = output_grad(branch, ctx_parts[2], out_proj, moved)
    dctx_parts = [mine] + [mp_swap(sends[k - 1], k) for k in (3, 2, 1)]
    pulled, squares = values_grad(dctx_parts, probs, gram, width)
    grad = weight_grad(turned, pulled)
    squares = squares + sum(mp_swap(squares, k) for k in (3, 2, 1))
    new_local = inner_update(grad, value_proj, squares, width * cols * groups)
    return (new_outer, new_momentum, new_local[None])


def solution(mesh):
    fine = Mesh(mesh.devices.reshape(2, 4, 4, 2, 4), (*OWNERS, "mp"))
    placed = (
        P(OWNERS, None, None, "mp"),
        P(None, OWNERS, "mp"),
        P(None, OWNERS, "mp"),
        P(OWNERS, "mp"),
        P(OWNERS, "mp"),
        P(OWNERS, "mp"),
        P(OWNERS),
    )

    return jax.shard_map(
        shards,
        mesh=fine,
        in_specs=placed,
        out_specs=(P(None, OWNERS, "mp"), P(None, OWNERS, "mp"), P(OWNERS, None, "mp")),
        check_vma=False,
    )
```
